128 devices in a mesh: rep: 2 (over z_hi), shard: 64 (over y, z_lo, x, core).
Axes of the slice: x: 4, y: 4, z: 4 (z_hi: 2, z_lo: 2; z = z_hi * 2 + z_lo), core: 2. Of those that a mesh axis runs over, the one named last changes fastest.
Arguments:
- dense: bfloat16 [32768, 128], P(('rep', 'shard')), may hold values from -6 to 6
- small_ids: int32 [32768, 32], P(('rep', 'shard')), may hold values from 0 to 511
- labels: int32 [32768], P(('rep', 'shard')), may hold values 0 or 1
- small_tables: bfloat16 [32, 512, 128], replicated, may hold values from -6 to 6
- large_tables: bfloat16 [64, 8192, 128], P('shard'), may hold values from -6 to 6
- batch_sizes: int32 [64, 128], replicated, may hold values from 1 to 128, as said below
- bag_ends: int32 [64, 128, 128], P('shard'), may hold values from 0 to 256, as said below
- owner_row_index: int32 [64, 128, 256], P('shard'), may hold values from 0 to 8191
- w_first: bfloat16 [4784, 1024], replicated, may hold values from -0.09375 to 0.09375
- b_first: float32 [1024], replicated, may hold values from -3 to 3
- w_out: float32 [1024], replicated, may hold values from -0.1875 to 0.1875
Outputs:
- small_new: bfloat16 [32, 512, 128], replicated
- large_new: bfloat16 [64, 8192, 128], P('shard')
The draws below stay inside these ranges and needn't reach their ends.
Inputs may be any that keep to these rules, and one draw needn't show every extreme that they name: `batch_sizes`: every feature has some owner, and every owner some feature, with exactly 128. `bag_ends`: nondecreasing along the last dimension; bags j >= batch_sizes[f, d] are empty; some bag list reaches 256.
All inputs are finite; a program needn't handle non-finite values. No bound on the sum of `labels` on one device may be relied on, other than what follows from the above.
Results may differ from the reference program's by a relative error of at most 0.0095.
Values may be sent and summed in bfloat16 or wider, within the bound.
A program may use at most 192 MiB of HBM per device.

```python
import math
import jax
import jax.numpy as jnp
import numpy as np
from jax import lax

E = 128
SROWS = 512
NSMALL = 32
LROWS = 8192
HID1 = 1024
PMAX = 3
BATCH = 256
BSMAX = 128
SLOTS = 256
FEAT = 64
DEST = 128
ROWS = 32768
PAIRS = 4656


def batch_table(key):
    folded = jax.random.fold_in(key, 7301)
    first_key, second_key, third_key = jax.random.split(folded, 3)
    size_table = jax.random.randint(first_key, (FEAT, DEST), 1, BSMAX + 1)
    pick_feature = jax.random.randint(second_key, (DEST,), 0, FEAT)
    pick_owner = jax.random.randint(third_key, (FEAT,), 0, DEST)
    forced = (jnp.arange(FEAT)[:, None] == pick_feature[None, :]) | (jnp.arange(DEST)[None, :] == pick_owner[:, None])
    return jnp.where(forced, BSMAX, size_table).astype(jnp.int32)


def draw_batch_sizes(key, part):
    return batch_table(key)


def draw_bag_ends(key, part):
    size_table = batch_table(key)
    lengths = jax.random.randint(jax.random.fold_in(key, 7302), (FEAT, DEST, BSMAX), 1, PMAX + 1)
    lengths = jnp.where(size_table[:, :, None] == BSMAX, PMAX, lengths)
    active = jnp.arange(BSMAX)[None, None, :] < size_table[:, :, None]
    limits = jnp.cumsum(jnp.where(active, lengths, 0), axis=2)
    return jnp.minimum(limits, SLOTS).astype(jnp.int32)


def touch_ends(result, stream_key, smallest, top_value):
    place = [jax.random.randint(jax.random.fold_in(stream_key, axis), (), 0, length) for axis, length in enumerate(result.shape)]
    widest = result.shape.index(max(result.shape))
    neighbour = place[:widest] + [(place[widest] + 1) % result.shape[widest]] + place[widest + 1:]
    return result.at[tuple(place)].set(smallest).at[tuple(neighbour)].set(top_value)


def block_levels(own_key, dims, cuts, least, largest):
    gain, own = 1.0, jax.random.fold_in(own_key, 6)
    for position, blocks in cuts:
        heights = jnp.exp(jax.random.uniform(jax.random.fold_in(own, position), (blocks,), jnp.float32, least / len(cuts), largest / len(cuts)))
        gain = gain * jnp.repeat(heights, dims[position] // blocks).reshape([-1 if axis == position else 1 for axis in range(len(dims))])
    return gain


def rank_table(amount, lean):
    weights = [(1 << 20) // math.isqrt(standing ** lean) + 1 for standing in range(1, amount + 1)]
    deviation = 1 + sum(weights) // (1 << 30)
    return np.cumsum(np.array([max(1, weight // deviation) for weight in weights]))


def skewed_ids(own_key, shape, amount, lean):
    grid = rank_table(amount, lean)
    ticket = jax.random.randint(jax.random.fold_in(own_key, 1), shape, 0, int(grid[amount - 1]))
    grade = jnp.searchsorted(jnp.asarray(grid, jnp.int32), ticket, side="right")
    return jax.random.permutation(jax.random.fold_in(own_key, 2), amount)[grade].astype(jnp.int32)


def normal_values(rng, shape, spread, bound, shards=(), held_as=jnp.bfloat16):
    entries = jax.random.normal(rng, shape, jnp.float32) * spread
    if len(shards) > 0:
        entries = block_levels(rng, shape, shards, -0.22, 0.18) * entries
    return jnp.clip(entries, min=-bound, max=bound).astype(held_as)


def setup_inputs(seed: int = 0) -> dict:
    splits = jax.random.split(jax.random.key(seed), 12)
    return {
        "dense": normal_values(splits[0], (ROWS, E), 1.0, 6.0, ((0, 128),)),
        "small_ids": touch_ends(jax.random.randint(splits[1], (ROWS, NSMALL), 0, SROWS), jax.random.fold_in(splits[1], 1), 0, SROWS - 1).astype(jnp.int32),
        "labels": touch_ends((jax.random.randint(splits[2], (ROWS,), 0, 4) < 1).astype(jnp.int32), jax.random.fold_in(splits[2], 1), 0, 1),
        "small_tables": normal_values(splits[3], (NSMALL, SROWS, E), 1.0, 6.0),
        "large_tables": normal_values(splits[4], (FEAT, LROWS, E), 1.0, 6.0, ((0, 64),)),
        "batch_sizes": draw_batch_sizes(jax.random.fold_in(splits[11], 71), 0),
        "bag_ends": draw_bag_ends(jax.random.fold_in(splits[11], 71), 0),
        "owner_row_index": touch_ends(skewed_ids(splits[7], (FEAT, DEST, SLOTS), LROWS, 2), jax.random.fold_in(splits[7], 3), 0, LROWS - 1).astype(jnp.int32),
        "w_first": normal_values(splits[8], (PAIRS + E, HID1), (PAIRS + E) ** -0.5, 0.09375),
        "b_first": normal_values(splits[9], (HID1,), 0.5, 3.0, (), jnp.float32),
        "w_out": normal_values(splits[10], (HID1,), HID1 ** -0.5, 0.1875, (), jnp.float32),
    }


step_size = 32.0

def bag_members(limits):
    starts = jnp.concatenate([jnp.zeros(limits.shape[:-1] + (1,), jnp.int32), limits[..., :-1]], axis=-1)
    positions = jnp.arange(SLOTS, dtype=jnp.int32)
    inside = (positions >= starts[..., None]) & (positions < limits[..., None])
    return inside.astype(jnp.float32)

def silu_slope(preacts):
    squash = jax.nn.sigmoid(preacts)
    return squash * (1.0 + preacts * (1.0 - squash))

def reference(dense, small_ids, labels, small_tables, large_tables, batch_sizes, bag_ends, owner_row_index, w_first, b_first, w_out):
    vec_count = 1 + NSMALL + FEAT
    lower_rows, lower_cols = np.tril_indices(vec_count, -1)

    def pool_one(packed):
        table_one, row_list, limits = packed
        bag_entry = bag_members(limits)
        collected_rows = table_one[row_list].astype(jnp.float32)
        return jnp.einsum('hxt,htv->hxv', bag_entry, collected_rows).astype(jnp.bfloat16)
    pooled = lax.map(pool_one, (large_tables, owner_row_index, bag_ends))
    pooled_dev = jnp.moveaxis(pooled, 1, 0)
    dense_blocks = dense.reshape(DEST, BATCH, E)
    id_blocks = small_ids.reshape(DEST, BATCH, NSMALL)
    label_blocks = labels.reshape(DEST, BATCH).astype(jnp.float32)
    size_blocks = jnp.transpose(batch_sizes)
    samples = jnp.arange(BATCH, dtype=jnp.int32)
    table_offsets = jnp.arange(NSMALL, dtype=jnp.int32) * SROWS
    feat_offsets = jnp.arange(FEAT, dtype=jnp.int32) * BSMAX

    def device_step(totals, inputs):
        dense_b, ids_b, label_b, pooled_b, size_row = inputs
        chosen = samples[None, :] * size_row[:, None] // BATCH
        large_feat = jnp.take_along_axis(pooled_b, chosen[:, :, None].astype(jnp.int32), axis=1)
        large_feat = jnp.transpose(large_feat, (1, 0, 2))
        minor_feature = small_tables[jnp.arange(NSMALL)[None, :], ids_b]
        vectors = jnp.concatenate([dense_b[:, None, :], minor_feature, large_feat], axis=1)
        vec_float = vectors.astype(jnp.float32)
        gram_matrix = jnp.einsum('bie,bje->bij', vec_float, vec_float)
        pair_values = (gram_matrix[:, lower_rows, lower_cols] * E ** (-0.5)).astype(jnp.bfloat16)
        features = jnp.concatenate([pair_values, dense_b], axis=1)
        preact = jnp.dot(features, w_first, preferred_element_type=jnp.float32) + b_first
        hidden = jax.nn.silu(preact)
        logits = lax.optimization_barrier(jnp.sum(hidden * w_out[None, :], axis=1))
        logit_grad = jax.nn.sigmoid(logits) - label_b
        pre_grad = (logit_grad[:, None] * w_out[None, :] * silu_slope(preact)).astype(jnp.bfloat16)
        pair_grad = jnp.dot(pre_grad, jnp.transpose(w_first[:PAIRS]), preferred_element_type=jnp.float32) * E ** (-0.5)
        lower_part = jnp.zeros((BATCH, vec_count, vec_count), jnp.float32).at[:, lower_rows, lower_cols].set(pair_grad)
        vec_grad = jnp.einsum('bij,bje->bie', lower_part + jnp.swapaxes(lower_part, 1, 2), vec_float).astype(jnp.bfloat16)
        small_part = vec_grad[:, 1:1 + NSMALL].astype(jnp.float32).reshape(-1, E)
        small_index = (table_offsets[None, :] + ids_b).reshape(-1).astype(jnp.int32)
        totals = totals + jax.ops.segment_sum(small_part, small_index, NSMALL * SROWS)
        large_part = jnp.transpose(vec_grad[:, 1 + NSMALL:], (1, 0, 2)).astype(jnp.float32).reshape(-1, E)
        large_index = (feat_offsets[:, None] + chosen).reshape(-1).astype(jnp.int32)
        accumulate_gradient = jax.ops.segment_sum(large_part, large_index, FEAT * BSMAX).reshape(FEAT, BSMAX, E).astype(jnp.bfloat16)
        return (totals, accumulate_gradient)
    start_totals = jnp.zeros((NSMALL * SROWS, E), jnp.float32)
    small_grad, fold_all = lax.scan(device_step, start_totals, (dense_blocks, id_blocks, label_blocks, pooled_dev, size_blocks))
    fold_feat = jnp.moveaxis(fold_all, 0, 1)

    def table_grad(packed):
        row_list, limits, gradient_list = packed
        bag_entry = bag_members(limits)
        slot_vectors = jnp.einsum('bni,bnv->biv', bag_entry, gradient_list.astype(jnp.float32))
        return jax.ops.segment_sum(slot_vectors.reshape(-1, E), row_list.reshape(-1).astype(jnp.int32), LROWS)
    large_grad = lax.map(table_grad, (owner_row_index, bag_ends, fold_feat))
    small_new = (small_tables.astype(jnp.float32) - step_size * small_grad.reshape(NSMALL, SROWS, E)).astype(jnp.bfloat16)
    large_new = (large_tables.astype(jnp.float32) - step_size * large_grad).astype(jnp.bfloat16)
    return (small_new, large_new)
```

```python
import functools
import jax
import jax.numpy as jnp
from jax import lax
from jax.experimental import pallas as pl
from jax.experimental.pallas import tpu as pltpu
from jax.sharding import Mesh, PartitionSpec as P

step_size = 32.0
LANES = 128
VMEM_CAP = 67_000_000
F32 = jnp.float32
BF16 = jnp.bfloat16

OWNERS = ("y", "zl", "x", "core")
ALL = ("rep",) + OWNERS
PLANE = ("rep", "y", "zl", "core")


def whole(space=pltpu.VMEM):
    return pl.BlockSpec(memory_space=space)


def bag_mask(ends_row, slots):
    bags = ends_row.shape[1]
    lane = lax.broadcasted_iota(jnp.int32, (1, bags), 1)
    starts = jnp.where(lane == 0, 0, pltpu.roll(ends_row, 1, 1))
    slot = lax.broadcasted_iota(jnp.int32, (slots, bags), 0)
    inside = (slot >= starts) & (slot < ends_row)
    return jnp.where(inside, 1.0, 0.0).astype(BF16)


def pool_kernel(ids, used, ends, table, out, wide, rows, *, group, unroll):
    dests, bags = ends.shape
    slots = ids.shape[1]
    wide[...] = table[...].astype(F32)
    rows[...] = jnp.zeros(rows.shape, F32)

    def one_group(g, _):
        def one_dest(i, _):
            d = g * group + i
            base = i * slots

            def chunk(c, _):
                first = c * unroll
                for u in range(unroll):
                    rows[pl.ds(base + first + u, 1), :] = wide[pl.ds(ids[d, first + u], 1), :]
                return 0

            lax.fori_loop(0, (used[d] + unroll - 1) // unroll, chunk, 0)
            return 0

        lax.fori_loop(0, group, one_dest, 0)
        limits = ends[pl.ds(pl.multiple_of(g * group, group), group), :]
        for i in range(group):
            mask = bag_mask(limits[i : i + 1], slots)
            taken = rows[i * slots : (i + 1) * slots, :].astype(BF16)
            total = lax.dot_general(
                mask, taken, (((0,), (0,)), ((), ())), preferred_element_type=F32
            )
            out[g * group + i] = total.astype(BF16)
        return 0

    lax.fori_loop(0, dests // group, one_group, 0)


def pool(ids, used, ends, table):
    dests, bags = ends.shape
    slots = ids.shape[1]
    group = 8
    return pl.pallas_call(
        functools.partial(pool_kernel, group=group, unroll=16),
        out_shape=jax.ShapeDtypeStruct((dests, bags, LANES), BF16),
        in_specs=[whole(pltpu.SMEM), whole(pltpu.SMEM), whole(), whole()],
        out_specs=whole(),
        scratch_shapes=[
            pltpu.VMEM(table.shape, F32),
            pltpu.VMEM((group * slots, LANES), F32),
        ],
        compiler_params=pltpu.CompilerParams(vmem_limit_bytes=VMEM_CAP),
        name="pool",
    )(ids, used, ends, table)


def scatter_kernel(ids, used, ends, folds, table, out, vals, *accs, group, unroll):
    dests, bags = ends.shape
    slots = ids.shape[1]
    ways = len(accs)
    for acc in accs:
        acc[...] = jnp.zeros(acc.shape, F32)

    def one_group(g, _):
        limits = ends[pl.ds(pl.multiple_of(g * group, group), group), :]
        for i in range(group):
            mask = bag_mask(limits[i : i + 1], slots)
            vals[i * slots : (i + 1) * slots, :] = jnp.dot(
                mask, folds[g * group + i], preferred_element_type=F32
            )

        def one_dest(i, _):
            d = g * group + i
            base = i * slots

            def chunk(c, _):
                first = c * unroll
                for v in range(0, unroll, ways):
                    spots = [ids[d, first + v + w] for w in range(ways)]
                    sums = [
                        accs[w][pl.ds(spots[w], 1), :] + vals[pl.ds(base + first + v + w, 1), :]
                        for w in range(ways)
                    ]
                    for w in range(ways):
                        accs[w][pl.ds(spots[w], 1), :] = sums[w]
                return 0

            lax.fori_loop(0, (used[d] + unroll - 1) // unroll, chunk, 0)
            return 0

        lax.fori_loop(0, group, one_dest, 0)
        return 0

    lax.fori_loop(0, dests // group, one_group, 0)

    def finish(c, _):
        span = pl.ds(pl.multiple_of(c * 128, 128), 128)
        total = accs[0][span, :]
        for acc in accs[1:]:
            total = total + acc[span, :]
        out[span, :] = (table[span, :].astype(F32) - step_size * total).astype(BF16)
        return 0

    lax.fori_loop(0, table.shape[0] // 128, finish, 0)


def scatter(ids, used, ends, folds, table, ways=4):
    slots = ids.shape[1]
    group = 8
    return pl.pallas_call(
        functools.partial(scatter_kernel, group=group, unroll=16),
        out_shape=jax.ShapeDtypeStruct(table.shape, BF16),
        in_specs=[whole(pltpu.SMEM), whole(pltpu.SMEM), whole(), whole(), whole()],
        out_specs=whole(),
        scratch_shapes=[pltpu.VMEM((group * slots, LANES), F32)]
        + [pltpu.VMEM(table.shape, F32)] * ways,
        compiler_params=pltpu.CompilerParams(vmem_limit_bytes=VMEM_CAP),
        name="scatter",
    )(ids, used, ends, folds, table)


def top_kernel(
    sizes, arrived, small, dense, labels, w_first, b_first, w_out,
    small_out, fold_out,
    vec, gram, feats, preact, pre_grad, pair_grad,
    *, pitch, vec_count,
):
    feat_count, bags, width = arrived.shape
    small_count, batch, _ = small.shape
    shift = batch.bit_length() - 1
    pairs = vec_count * (vec_count - 1) // 2
    scale = width ** (-0.5)
    hidden = w_first.shape[1]
    first_large = 1 + small_count

    def column(row, count=batch, first=0):
        return pl.ds(first * pitch + row, count, stride=pitch)

    for row in range(vec_count, pitch):
        vec[column(row), :] = jnp.zeros((batch, width), F32)
    vec[batch * pitch :, :] = jnp.zeros((vec.shape[0] - batch * pitch, width), F32)
    vec[column(0), :] = dense[...].astype(F32)
    for t in range(small_count):
        vec[column(1 + t), :] = small[t].astype(F32)
    sample = lax.broadcasted_iota(jnp.int32, (batch, bags), 0)
    bag = lax.broadcasted_iota(jnp.int32, (batch, bags), 1)
    for f in range(feat_count):
        hot = jnp.where(((sample * sizes[f]) >> shift) == bag, 1.0, 0.0).astype(BF16)
        vec[column(first_large + f), :] = jnp.dot(hot, arrived[f], preferred_element_type=F32)

    together = 8

    def gram_step(s, _):
        base = s * (together * pitch)
        blocks = [
            vec[pl.ds(pl.multiple_of(base + n * pitch, 8), pitch), :].astype(BF16)
            for n in range(together)
        ]
        for n in range(together):
            g = lax.dot_general(
                blocks[n], blocks[n], (((1,), (1,)), ((), ())), preferred_element_type=F32
            )
            gram[pl.ds(pl.multiple_of(base + n * pitch, 8), pitch), 0:pitch] = g * scale
        return 0

    lax.fori_loop(0, batch // together, gram_step, 0)

    part = 64
    lane = lax.broadcasted_iota(jnp.int32, (part, LANES), 1)

    def pack_step(s, _):
        rows = pl.ds(pl.multiple_of(s * part, part), part)
        tile = None
        offset = 0
        for i in range(1, vec_count + 1):
            if i < vec_count:
                piece = gram[pl.ds(s * (part * pitch) + i, part, stride=pitch), :]
                length = i
            else:
                piece = dense[rows, :].astype(F32)
                length = width
            turn = offset % LANES
            number = offset // LANES
            if turn:
                piece = pltpu.roll(piece, turn, 1)
                tile = jnp.where(lane >= turn, piece, tile)
            else:
                tile = piece
            offset += length
            if offset // LANES > number:
                feats[rows, number * LANES : (number + 1) * LANES] = tile.astype(BF16)
                tile = piece
        if offset % LANES:
            number = offset // LANES
            feats[rows, number * LANES : (number + 1) * LANES] = tile.astype(BF16)
        return 0

    lax.fori_loop(0, batch // part, pack_step, 0)

    depth = pairs + width
    bulk = depth // LANES * LANES
    wide = 256
    for n in range(0, hidden, wide):
        total = jnp.dot(feats[:, :bulk], w_first[:bulk, n : n + wide], preferred_element_type=F32)
        total = total + jnp.dot(
            feats[:, bulk:depth], w_first[bulk:depth, n : n + wide], preferred_element_type=F32
        )
        preact[:, n : n + wide] = total + b_first[:, n : n + wide]

    def head_step(s, _):
        rows = pl.ds(pl.multiple_of(s * 16, 16), 16)
        v = preact[rows, :]
        squash = jax.nn.sigmoid(v)
        logit = jnp.sum(v * squash * w_out[...], axis=1, keepdims=True)
        logit_grad = jax.nn.sigmoid(logit) - labels[rows, :].astype(F32)
        slope = squash * (1.0 + v * (1.0 - squash))
        pre_grad[rows, :] = (logit_grad * w_out[...] * slope).astype(BF16)
        return 0

    lax.fori_loop(0, batch // 16, head_step, 0)

    bulk = pairs // wide * wide
    for n in range(0, pairs, wide):
        span = min(wide, pairs - n)
        g = lax.dot_general(
            pre_grad[...], w_first[n : n + span, :], (((1,), (1,)), ((), ())),
            preferred_element_type=F32,
        )
        pair_grad[:, n : n + span] = g * scale

    def unpack_step(s, _):
        rows = pl.ds(pl.multiple_of(s * part, part), part)
        offset = 0
        for i in range(pitch):
            where_to = pl.ds(s * (part * pitch) + i, part, stride=pitch)
            if i == 0 or i >= vec_count:
                gram[where_to, :] = jnp.zeros((part, LANES), F32)
                continue
            turn = offset % LANES
            number = offset // LANES
            back = (LANES - turn) % LANES
            piece = pair_grad[rows, number * LANES : (number + 1) * LANES]
            if back:
                piece = pltpu.roll(piece, back, 1)
            if turn + i > LANES:
                more = pair_grad[rows, (number + 1) * LANES : (number + 2) * LANES]
                piece = jnp.where(lane < LANES - turn, piece, pltpu.roll(more, back, 1))
            gram[where_to, :] = jnp.where(lane < i, piece, 0.0)
            offset += i
        return 0

    lax.fori_loop(0, batch // part, unpack_step, 0)

    def grad_step(s, _):
        base = s * (together * pitch)
        found = []
        for n in range(together):
            spot = pl.multiple_of(base + n * pitch, 8)
            lower = gram[pl.ds(spot, pitch), :].astype(BF16)
            vectors = vec[pl.ds(spot, LANES), :].astype(BF16)
            found.append((lower, vectors))
        for n in range(together):
            lower, vectors = found[n]
            spot = pl.multiple_of(base + n * pitch, 8)
            one = jnp.dot(lower, vectors, preferred_element_type=F32)
            two = lax.dot_general(
                lower, vectors[:pitch], (((0,), (0,)), ((), ())), preferred_element_type=F32
            )
            vec[pl.ds(spot, pitch), :] = one + two[:pitch]
        return 0

    lax.fori_loop(0, batch // together, grad_step, 0)

    for t in range(small_count):
        small_out[t] = vec[column(1 + t), :].astype(BF16)
    sample_t = lax.broadcasted_iota(jnp.int32, (bags, batch), 1)
    bag_t = lax.broadcasted_iota(jnp.int32, (bags, batch), 0)
    for f in range(feat_count):
        hot = jnp.where(((sample_t * sizes[f]) >> shift) == bag_t, 1.0, 0.0).astype(BF16)
        grads = vec[column(first_large + f), :].astype(BF16)
        fold = jnp.dot(hot, grads, preferred_element_type=F32).astype(BF16)
        for copy in range(fold_out.shape[0]):
            fold_out[copy, f] = fold


def top(sizes, arrived, small, dense, labels, w_first, b_first, w_out, copies):
    feat_count, bags, width = arrived.shape
    small_count, batch, _ = small.shape
    vec_count = 1 + small_count + feat_count
    pitch = -(-vec_count // 8) * 8
    pairs = vec_count * (vec_count - 1) // 2
    depth = pairs + width
    hidden = w_first.shape[1]

    def up(n):
        return -(-n // LANES) * LANES

    return pl.pallas_call(
        functools.partial(top_kernel, pitch=pitch, vec_count=vec_count),
        out_shape=(
            jax.ShapeDtypeStruct((small_count, batch, width), BF16),
            jax.ShapeDtypeStruct((copies, feat_count, bags, width), BF16),
        ),
        in_specs=[whole(pltpu.SMEM)] + [whole()] * 7,
        out_specs=(whole(), whole()),
        scratch_shapes=[
            pltpu.VMEM((batch * pitch + LANES - pitch, width), F32),
            pltpu.VMEM((batch * pitch, LANES), F32),
            pltpu.VMEM((batch, up(depth)), BF16),
            pltpu.VMEM((batch, hidden), F32),
            pltpu.VMEM((batch, hidden), BF16),
            pltpu.VMEM((batch, up(pairs)), F32),
        ],
        compiler_params=pltpu.CompilerParams(vmem_limit_bytes=VMEM_CAP),
        name="top",
    )(sizes, arrived, small, dense, labels, w_first, b_first, w_out)


def shards(
    dense, small_ids, labels, small_tables, large_tables,
    batch_sizes, bag_ends, owner_row_index, w_first, b_first, w_out,
):
    groups = 1
    for name in OWNERS:
        groups = groups * lax.axis_size(name)
    copies = lax.axis_size("rep")
    replica = lax.axis_index("rep")
    me = lax.axis_index(ALL)
    first = replica * groups
    small_rows = small_tables.shape[1]
    table = large_tables[0]
    ends, ids = bag_ends[0], owner_row_index[0]
    used = ends[:, -1]
    slots = ids.shape[1]

    def mine(a):
        return lax.dynamic_slice_in_dim(a, first, groups, 0)

    ids_sent = lax.all_to_all(small_ids.T[:, None], PLANE, 0, 0, tiled=True)
    sizes = lax.dynamic_slice_in_dim(batch_sizes, me, 1, 1)[:, 0]

    pooled = pool(mine(ids), mine(used), mine(ends), table)
    arrived = lax.all_to_all(pooled, OWNERS, 0, 0, tiled=True)
    hot = (small_ids.T[:, :, None] == jnp.arange(small_rows, dtype=jnp.int32)).astype(BF16)
    small = jnp.einsum("tbr,tre->tbe", hot, small_tables, preferred_element_type=F32).astype(BF16)

    small_grad, folded = top(
        sizes, arrived, small, dense, labels[:, None], w_first, b_first[None], w_out[None], copies
    )

    grads = lax.all_to_all(small_grad, PLANE, 0, 0, tiled=True).reshape(-1, LANES)
    owner_hot = (ids_sent.reshape(-1)[:, None] == jnp.arange(small_rows, dtype=jnp.int32)).astype(BF16)
    partial = jnp.einsum("sr,se->re", owner_hot, grads, preferred_element_type=F32)
    total = lax.all_gather(partial, "x").sum(0)
    table_index = lax.axis_index(PLANE)
    mine_small = lax.dynamic_slice_in_dim(small_tables, table_index, 1, 0)[0]
    new_small = (mine_small.astype(F32) - step_size * total).astype(BF16)
    small_new = lax.all_gather(new_small, PLANE)

    folds = lax.all_to_all(folded.reshape((-1,) + folded.shape[2:]), ALL, 0, 0, tiled=True)
    large_new = scatter(ids, used, ends, folds, table)
    return small_new, large_new[None]


def solution(mesh):
    fine = Mesh(mesh.devices.reshape(2, 4, 2, 4, 2), ALL)
    placed = (
        P(ALL, None), P(ALL, None), P(ALL), P(), P(OWNERS, None, None), P(),
        P(OWNERS, None, None), P(OWNERS, None, None), P(), P(), P(),
    )
    return jax.shard_map(
        shards, mesh=fine, in_specs=placed, out_specs=(P(), P(OWNERS, None, None)), check_vma=False
    )
```

```python
import functools
import jax
import jax.numpy as jnp
from jax import lax
from jax.experimental import pallas as pl
from jax.experimental.pallas import tpu as pltpu
from jax.sharding import Mesh, PartitionSpec as P

step_size = 32.0
LANES = 128
VMEM_CAP = 67_000_000
F32 = jnp.float32
BF16 = jnp.bfloat16

OWNERS = ("y", "zl", "x", "core")
ALL = ("rep",) + OWNERS
PLANE = ("rep", "y", "zl", "core")


def whole(space=pltpu.VMEM):
    return pl.BlockSpec(memory_space=space)


def bag_mask(ends_row, slots):
    bags = ends_row.shape[1]
    lane = lax.broadcasted_iota(jnp.int32, (1, bags), 1)
    starts = jnp.where(lane == 0, 0, pltpu.roll(ends_row, 1, 1))
    slot = lax.broadcasted_iota(jnp.int32, (slots, bags), 0)
    inside = (slot >= starts) & (slot < ends_row)
    return jnp.where(inside, 1.0, 0.0).astype(BF16)


def cost(micros):
    return pl.CostEstimate(flops=0, bytes_accessed=int(micros * 3.0e6), transcendentals=0)


def slot_base(d, k, slots):
    return (((d >> 3) * (slots // 128) + (k >> 7)) << 10) + ((d & 7) << 7) + (k & 127)


def pool_kernel(first, ids, flat_ends, ends, table, out, wide, rows, *, group, unroll, slots):
    dests, bags, _ = out.shape
    wide[...] = table[...].astype(F32)
    rows[...] = jnp.zeros(rows.shape, F32)

    def one_group(g, _):
        def one_dest(i, _):
            d = first[0] + g * group + i
            row = i * slots

            def chunk(c, _):
                start = slot_base(d, c * unroll, slots)
                place = row + c * unroll
                for u in range(unroll):
                    rows[pl.ds(place + u, 1), :] = wide[pl.ds(ids[start + u], 1), :]
                return 0

            used = flat_ends[d * bags + bags - 1]
            lax.fori_loop(0, (used + unroll - 1) >> (unroll.bit_length() - 1), chunk, 0)
            return 0

        lax.fori_loop(0, group, one_dest, 0)
        limits = ends[pl.ds(pl.multiple_of(first[0] + g * group, group), group), :]
        for i in range(group):
            mask = bag_mask(limits[i : i + 1], slots)
            taken = rows[i * slots : (i + 1) * slots, :].astype(BF16)
            total = lax.dot_general(
                mask, taken, (((0,), (0,)), ((), ())), preferred_element_type=F32
            )
            out[g * group + i] = total.astype(BF16)
        return 0

    lax.fori_loop(0, dests // group, one_group, 0)


def pool(first, ids, flat_ends, ends, table, dests, slots):
    bags = ends.shape[1]
    group = 8
    return pl.pallas_call(
        functools.partial(pool_kernel, group=group, unroll=32, slots=slots),
        out_shape=jax.ShapeDtypeStruct((dests, bags, LANES), BF16),
        in_specs=[whole(pltpu.SMEM)] * 3 + [whole()] * 2,
        out_specs=whole(),
        scratch_shapes=[
            pltpu.VMEM(table.shape, F32),
            pltpu.VMEM((group * slots, LANES), F32),
        ],
        compiler_params=pltpu.CompilerParams(vmem_limit_bytes=VMEM_CAP),
        cost_estimate=cost(16),
        name="pool",
    )(first, ids, flat_ends, ends, table)


def scatter_kernel(ids, flat_ends, ends, folds, table, out, vals, *accs, group, unroll, slots):
    dests, bags = ends.shape
    ways = len(accs)
    for acc in accs:
        acc[...] = jnp.zeros(acc.shape, F32)

    def one_group(g, _):
        limits = ends[pl.ds(pl.multiple_of(g * group, group), group), :]
        for i in range(group):
            mask = bag_mask(limits[i : i + 1], slots)
            vals[i * slots : (i + 1) * slots, :] = jnp.dot(
                mask, folds[g * group + i], preferred_element_type=F32
            )

        def one_dest(i, _):
            d = g * group + i
            row = i * slots

            def chunk(c, _):
                start = slot_base(d, c * unroll, slots)
                place = row + c * unroll
                for v in range(0, unroll, ways):
                    spots = [ids[start + v + w] for w in range(ways)]
                    sums = [
                        accs[w][pl.ds(spots[w], 1), :] + vals[pl.ds(place + v + w, 1), :]
                        for w in range(ways)
                    ]
                    for w in range(ways):
                        accs[w][pl.ds(spots[w], 1), :] = sums[w]
                return 0

            used = flat_ends[d * bags + bags - 1]
            lax.fori_loop(0, (used + unroll - 1) >> (unroll.bit_length() - 1), chunk, 0)
            return 0

        lax.fori_loop(0, group, one_dest, 0)
        return 0

    lax.fori_loop(0, dests // group, one_group, 0)

    def finish(c, _):
        span = pl.ds(pl.multiple_of(c * 128, 128), 128)
        total = accs[0][span, :]
        for acc in accs[1:]:
            total = total + acc[span, :]
        out[span, :] = (table[span, :].astype(F32) - step_size * total).astype(BF16)
        return 0

    lax.fori_loop(0, table.shape[0] // 128, finish, 0)


def scatter(ids, flat_ends, ends, folds, table, slots, ways=8):
    group = 8
    return pl.pallas_call(
        functools.partial(scatter_kernel, group=group, unroll=32, slots=slots),
        out_shape=jax.ShapeDtypeStruct(table.shape, BF16),
        in_specs=[whole(pltpu.SMEM)] * 2 + [whole()] * 3,
        out_specs=whole(),
        scratch_shapes=[pltpu.VMEM((group * slots, LANES), F32)]
        + [pltpu.VMEM(table.shape, F32)] * ways,
        compiler_params=pltpu.CompilerParams(vmem_limit_bytes=VMEM_CAP),
        cost_estimate=cost(28),
        name="scatter",
    )(ids, flat_ends, ends, folds, table)


def top_kernel(
    sizes, arrived, small, dense, labels, w_first, b_first, w_out,
    small_out, fold_out,
    vec, gram, feats, preact, pre_grad, pair_grad,
    *, pitch, vec_count,
):
    feat_count, bags, width = arrived.shape
    small_count, batch, _ = small.shape
    shift = batch.bit_length() - 1
    pairs = vec_count * (vec_count - 1) // 2
    scale = width ** (-0.5)
    hidden = w_first.shape[1]
    first_large = 1 + small_count

    def column(row, count=batch, first=0):
        return pl.ds(first * pitch + row, count, stride=pitch)

    for row in range(vec_count, pitch):
        vec[column(row), :] = jnp.zeros((batch, width), F32)
    vec[batch * pitch :, :] = jnp.zeros((vec.shape[0] - batch * pitch, width), F32)
    vec[column(0), :] = dense[...].astype(F32)
    for t in range(small_count):
        vec[column(1 + t), :] = small[t].astype(F32)
    sample = lax.broadcasted_iota(jnp.int32, (batch, bags), 0)
    bag = lax.broadcasted_iota(jnp.int32, (batch, bags), 1)
    for f in range(feat_count):
        hot = jnp.where(((sample * sizes[f]) >> shift) == bag, 1.0, 0.0).astype(BF16)
        vec[column(first_large + f), :] = jnp.dot(hot, arrived[f], preferred_element_type=F32)

    together = 8

    def gram_step(s, _):
        base = s * (together * pitch)
        blocks = [
            vec[pl.ds(pl.multiple_of(base + n * pitch, 8), pitch), :].astype(BF16)
            for n in range(together)
        ]
        for n in range(together):
            g = lax.dot_general(
                blocks[n], blocks[n], (((1,), (1,)), ((), ())), preferred_element_type=F32
            )
            gram[pl.ds(pl.multiple_of(base + n * pitch, 8), pitch), 0:pitch] = g * scale
        return 0

    lax.fori_loop(0, batch // together, gram_step, 0)

    part = 64
    lane = lax.broadcasted_iota(jnp.int32, (part, LANES), 1)

    def pack_step(s, _):
        rows = pl.ds(pl.multiple_of(s * part, part), part)
        tile = None
        offset = 0
        for i in range(1, vec_count + 1):
            if i < vec_count:
                piece = gram[pl.ds(s * (part * pitch) + i, part, stride=pitch), :]
                length = i
            else:
                piece = dense[rows, :].astype(F32)
                length = width
            turn = offset % LANES
            number = offset // LANES
            if turn:
                piece = pltpu.roll(piece, turn, 1)
                tile = jnp.where(lane >= turn, piece, tile)
            else:
                tile = piece
            offset += length
            if offset // LANES > number:
                feats[rows, number * LANES : (number + 1) * LANES] = tile.astype(BF16)
                tile = piece
        if offset % LANES:
            number = offset // LANES
            feats[rows, number * LANES : (number + 1) * LANES] = tile.astype(BF16)
        return 0

    lax.fori_loop(0, batch // part, pack_step, 0)

    depth = pairs + width
    bulk = depth // LANES * LANES
    wide = 256
    for n in range(0, hidden, wide):
        total = jnp.dot(feats[:, :bulk], w_first[:bulk, n : n + wide], preferred_element_type=F32)
        total = total + jnp.dot(
            feats[:, bulk:depth], w_first[bulk:depth, n : n + wide], preferred_element_type=F32
        )
        preact[:, n : n + wide] = total + b_first[:, n : n + wide]

    def head_step(s, _):
        rows = pl.ds(pl.multiple_of(s * 16, 16), 16)
        v = preact[rows, :]
        squash = jax.nn.sigmoid(v)
        logit = jnp.sum(v * squash * w_out[...], axis=1, keepdims=True)
        logit_grad = jax.nn.sigmoid(logit) - labels[rows, :].astype(F32)
        slope = squash * (1.0 + v * (1.0 - squash))
        pre_grad[rows, :] = (logit_grad * w_out[...] * slope).astype(BF16)
        return 0

    lax.fori_loop(0, batch // 16, head_step, 0)

    bulk = pairs // wide * wide
    for n in range(0, pairs, wide):
        span = min(wide, pairs - n)
        g = lax.dot_general(
            pre_grad[...], w_first[n : n + span, :], (((1,), (1,)), ((), ())),
            preferred_element_type=F32,
        )
        pair_grad[:, n : n + span] = g * scale

    def unpack_step(s, _):
        rows = pl.ds(pl.multiple_of(s * part, part), part)
        offset = 0
        for i in range(pitch):
            where_to = pl.ds(s * (part * pitch) + i, part, stride=pitch)
            if i == 0 or i >= vec_count:
                gram[where_to, :] = jnp.zeros((part, LANES), F32)
                continue
            turn = offset % LANES
            number = offset // LANES
            back = (LANES - turn) % LANES
            piece = pair_grad[rows, number * LANES : (number + 1) * LANES]
            if back:
                piece = pltpu.roll(piece, back, 1)
            if turn + i > LANES:
                more = pair_grad[rows, (number + 1) * LANES : (number + 2) * LANES]
                piece = jnp.where(lane < LANES - turn, piece, pltpu.roll(more, back, 1))
            gram[where_to, :] = jnp.where(lane < i, piece, 0.0)
            offset += i
        return 0

    lax.fori_loop(0, batch // part, unpack_step, 0)

    def grad_step(s, _):
        base = s * (together * pitch)
        found = []
        for n in range(together):
            spot = pl.multiple_of(base + n * pitch, 8)
            lower = gram[pl.ds(spot, pitch), :].astype(BF16)
            vectors = vec[pl.ds(spot, LANES), :].astype(BF16)
            found.append((lower, vectors))
        for n in range(together):
            lower, vectors = found[n]
            spot = pl.multiple_of(base + n * pitch, 8)
            one = jnp.dot(lower, vectors, preferred_element_type=F32)
            two = lax.dot_general(
                lower, vectors[:pitch], (((0,), (0,)), ((), ())), preferred_element_type=F32
            )
            vec[pl.ds(spot, pitch), :] = one + two[:pitch]
        return 0

    lax.fori_loop(0, batch // together, grad_step, 0)

    for t in range(small_count):
        small_out[t] = vec[column(1 + t), :].astype(BF16)
    sample_t = lax.broadcasted_iota(jnp.int32, (bags, batch), 1)
    bag_t = lax.broadcasted_iota(jnp.int32, (bags, batch), 0)
    for f in range(feat_count):
        hot = jnp.where(((sample_t * sizes[f]) >> shift) == bag_t, 1.0, 0.0).astype(BF16)
        grads = vec[column(first_large + f), :].astype(BF16)
        fold = jnp.dot(hot, grads, preferred_element_type=F32).astype(BF16)
        for copy in range(fold_out.shape[0]):
            fold_out[copy, f] = fold


def top(sizes, arrived, small, dense, labels, w_first, b_first, w_out, copies):
    feat_count, bags, width = arrived.shape
    small_count, batch, _ = small.shape
    vec_count = 1 + small_count + feat_count
    pitch = -(-vec_count // 8) * 8
    pairs = vec_count * (vec_count - 1) // 2
    depth = pairs + width
    hidden = w_first.shape[1]

    def up(n):
        return -(-n // LANES) * LANES

    return pl.pallas_call(
        functools.partial(top_kernel, pitch=pitch, vec_count=vec_count),
        out_shape=(
            jax.ShapeDtypeStruct((small_count, batch, width), BF16),
            jax.ShapeDtypeStruct((copies, feat_count, bags, width), BF16),
        ),
        in_specs=[whole(pltpu.SMEM)] + [whole()] * 7,
        out_specs=(whole(), whole()),
        scratch_shapes=[
            pltpu.VMEM((batch * pitch + LANES - pitch, width), F32),
            pltpu.VMEM((batch * pitch, LANES), F32),
            pltpu.VMEM((batch, up(depth)), BF16),
            pltpu.VMEM((batch, hidden), F32),
            pltpu.VMEM((batch, hidden), BF16),
            pltpu.VMEM((batch, up(pairs)), F32),
        ],
        compiler_params=pltpu.CompilerParams(vmem_limit_bytes=VMEM_CAP),
        cost_estimate=cost(45),
        name="top",
    )(sizes, arrived, small, dense, labels, w_first, b_first, w_out)


def step(
    dense, small_ids, labels, small_tables, large_tables,
    batch_sizes, bag_ends, owner_row_index, w_first, b_first, w_out,
):
    groups = 1
    for name in OWNERS:
        groups = groups * lax.axis_size(name)
    copies = lax.axis_size("rep")
    replica = lax.axis_index("rep")
    me = lax.axis_index(ALL)
    small_rows = small_tables.shape[1]
    table = large_tables[0]
    ends = bag_ends[0]
    slots = owner_row_index.shape[2]
    flat_ends = ends.reshape(-1)
    ids = owner_row_index.reshape(-1, 8, slots // 128, 128).transpose(0, 2, 1, 3).reshape(-1)
    first = (replica * groups).astype(jnp.int32).reshape(1)

    ids_sent = lax.all_to_all(small_ids.T[:, None], PLANE, 0, 0, tiled=True)
    sizes = lax.dynamic_slice_in_dim(batch_sizes, me, 1, 1)[:, 0]

    pooled = pool(first, ids, flat_ends, ends, table, groups, slots)
    arrived = lax.all_to_all(pooled, OWNERS, 0, 0, tiled=True)
    hot = (small_ids.T[:, :, None] == jnp.arange(small_rows, dtype=jnp.int32)).astype(BF16)
    small = jnp.einsum("tbr,tre->tbe", hot, small_tables, preferred_element_type=F32).astype(BF16)

    small_grad, folded = top(
        sizes, arrived, small, dense, labels[:, None], w_first, b_first[None], w_out[None], copies
    )

    grads = lax.all_to_all(small_grad, PLANE, 0, 0, tiled=True).reshape(-1, LANES)
    owner_hot = (ids_sent.reshape(-1)[:, None] == jnp.arange(small_rows, dtype=jnp.int32)).astype(BF16)
    partial = jnp.einsum("sr,se->re", owner_hot, grads, preferred_element_type=F32)
    total = lax.all_gather(partial, "x").sum(0)
    table_index = lax.axis_index(PLANE)
    mine_small = lax.dynamic_slice_in_dim(small_tables, table_index, 1, 0)[0]
    new_small = (mine_small.astype(F32) - step_size * total).astype(BF16)
    small_new = lax.all_gather(new_small, PLANE)

    folds = lax.all_to_all(folded.reshape((-1,) + folded.shape[2:]), ALL, 0, 0, tiled=True)
    large_new = scatter(ids, flat_ends, ends, folds, table, slots)
    return small_new, large_new[None]


def solution(mesh):
    fine = Mesh(mesh.devices.reshape(2, 4, 2, 4, 2), ALL)
    placed = (
        P(ALL, None), P(ALL, None), P(ALL), P(), P(OWNERS, None, None), P(),
        P(OWNERS, None, None), P(OWNERS, None, None), P(), P(), P(),
    )
    return jax.shard_map(
        step, mesh=fine, in_specs=placed, out_specs=(P(), P(OWNERS, None, None)), check_vma=False
    )
```

```python
import functools
import jax
import jax.numpy as jnp
from jax import lax
from jax.experimental import pallas as pl
from jax.experimental.pallas import tpu as pltpu
from jax.sharding import Mesh, PartitionSpec as P

step_size = 32.0
LANES = 128
WAYS = 8
VMEM_CAP = 67_000_000
F32 = jnp.float32
BF16 = jnp.bfloat16

OWNERS = ("y", "zl", "x", "core")
ALL = ("rep",) + OWNERS
PLANE = ("rep", "y", "zl", "core")


def whole(space=pltpu.VMEM):
    return pl.BlockSpec(memory_space=space)


def bag_mask(ends_row, slots, part, parts):
    bags = ends_row.shape[1]
    size = bags // parts
    lane = lax.broadcasted_iota(jnp.int32, (1, bags), 1)
    starts = jnp.where(lane == 0, 0, pltpu.roll(ends_row, 1, 1))
    if part:
        starts = pltpu.roll(starts, bags - part * size, 1)
        ends_row = pltpu.roll(ends_row, bags - part * size, 1)
    starts, ends_row = starts[:, :size], ends_row[:, :size]
    slot = lax.broadcasted_iota(jnp.int32, (slots, size), 0)
    inside = (slot >= starts) & (slot < ends_row)
    return jnp.where(inside, 1.0, 0.0).astype(BF16)


def slot_span(flat_ends, d, bags, part, parts, unroll):
    size = bags // parts
    step = unroll.bit_length() - 1
    low = flat_ends[d * bags + part * size - 1] >> step if part else 0
    return low, (flat_ends[d * bags + (part + 1) * size - 1] + unroll - 1) >> step


def cost(micros):
    return pl.CostEstimate(flops=0, bytes_accessed=int(micros * 3.0e6), transcendentals=0)


def slot_base(d, k, slots):
    return (((d >> 3) * (slots // 128) + (k >> 7)) << 10) + ((d & 7) << 7) + (k & 127)


def pool_kernel(first, ids, flat_ends, ends, table, out, wide, rows, *, group, unroll, slots, part, parts):
    dests = out.shape[0]
    bags = ends.shape[1]

    def widen(c, _):
        span = pl.ds(pl.multiple_of(c * 256, 256), 256)
        wide[span, :] = table[span, :].astype(F32)
        return 0

    lax.fori_loop(0, table.shape[0] // 256, widen, 0)
    rows[...] = jnp.zeros(rows.shape, F32)

    def one_group(g, _):
        def one_dest(i, _):
            d = first[0] + g * group + i
            row = i * slots

            def chunk(c, _):
                start = slot_base(d, c * unroll, slots)
                place = row + c * unroll
                for u in range(unroll):
                    rows[pl.ds(place + u, 1), :] = wide[pl.ds(ids[start + u], 1), :]
                return 0

            low, high = slot_span(flat_ends, d, bags, part, parts, unroll)
            lax.fori_loop(low, high, chunk, 0)
            return 0

        lax.fori_loop(0, group, one_dest, 0)
        limits = ends[pl.ds(pl.multiple_of(first[0] + g * group, group), group), :]
        for i in range(group):
            mask = bag_mask(limits[i : i + 1], slots, part, parts)
            taken = rows[i * slots : (i + 1) * slots, :].astype(BF16)
            total = lax.dot_general(
                mask, taken, (((0,), (0,)), ((), ())), preferred_element_type=F32
            )
            out[g * group + i] = total.astype(BF16)
        return 0

    lax.fori_loop(0, dests // group, one_group, 0)


def pool(first, ids, flat_ends, ends, table, dests, slots, part, parts):
    bags = ends.shape[1]
    group = 8
    return pl.pallas_call(
        functools.partial(
            pool_kernel, group=group, unroll=32, slots=slots, part=part, parts=parts
        ),
        out_shape=jax.ShapeDtypeStruct((dests, bags // parts, LANES), BF16),
        in_specs=[whole(pltpu.SMEM)] * 3 + [whole()] * 2,
        out_specs=whole(),
        scratch_shapes=[
            pltpu.VMEM(table.shape, F32),
            pltpu.VMEM((group * slots, LANES), F32),
        ],
        compiler_params=pltpu.CompilerParams(vmem_limit_bytes=VMEM_CAP),
        cost_estimate=cost(12),
        name="pool",
    )(first, ids, flat_ends, ends, table)


def scatter_kernel(ids, flat_ends, ends, folds, *rest, group, unroll, slots, part, parts, ways):
    before, table, out = (None, None) + rest[:1] if part == 0 else rest[:3]
    vals, *accs = rest[1 if part == 0 else 3 :]
    dests, bags = ends.shape

    def clear(c, _):
        for acc in accs:
            acc[pl.ds(pl.multiple_of(c * 128, 128), 128), :] = jnp.zeros((128, LANES), F32)
        return 0

    lax.fori_loop(0, out.shape[0] // 128, clear, 0)

    def one_group(g, _):
        limits = ends[pl.ds(pl.multiple_of(g * group, group), group), :]
        for i in range(group):
            mask = bag_mask(limits[i : i + 1], slots, part, parts)
            vals[i * slots : (i + 1) * slots, :] = jnp.dot(
                mask, folds[g * group + i], preferred_element_type=F32
            )

        def one_dest(i, _):
            d = g * group + i
            row = i * slots

            def chunk(c, _):
                start = slot_base(d, c * unroll, slots)
                place = row + c * unroll
                for v in range(0, unroll, ways):
                    spots = [ids[start + v + w] for w in range(ways)]
                    sums = [
                        accs[w][pl.ds(spots[w], 1), :] + vals[pl.ds(place + v + w, 1), :]
                        for w in range(ways)
                    ]
                    for w in range(ways):
                        accs[w][pl.ds(spots[w], 1), :] = sums[w]
                return 0

            low, high = slot_span(flat_ends, d, bags, part, parts, unroll)
            lax.fori_loop(low, high, chunk, 0)
            return 0

        lax.fori_loop(0, group, one_dest, 0)
        return 0

    lax.fori_loop(0, dests // group, one_group, 0)

    def finish(c, _):
        span = pl.ds(pl.multiple_of(c * 128, 128), 128)
        total = accs[0][span, :]
        for acc in accs[1:]:
            total = total + acc[span, :]
        if part:
            total = total + before[span, :]
        if part < parts - 1:
            out[span, :] = total
        else:
            out[span, :] = (table[span, :].astype(F32) - step_size * total).astype(BF16)
        return 0

    lax.fori_loop(0, out.shape[0] // 128, finish, 0)


def scatter(ids, flat_ends, ends, folds, before, table, slots, part, parts, ways):
    group = 8
    last = part == parts - 1
    extra = () if part == 0 else (before, table)
    return pl.pallas_call(
        functools.partial(
            scatter_kernel, group=group, unroll=32, slots=slots, part=part, parts=parts, ways=ways
        ),
        out_shape=jax.ShapeDtypeStruct(table.shape, BF16 if last else F32),
        in_specs=[whole(pltpu.SMEM)] * 2 + [whole()] * (2 + len(extra)),
        out_specs=whole(),
        scratch_shapes=[pltpu.VMEM((group * slots, LANES), F32)]
        + [pltpu.VMEM(table.shape, F32)] * ways,
        compiler_params=pltpu.CompilerParams(vmem_limit_bytes=VMEM_CAP),
        cost_estimate=cost(14 if last else 26),
        name="scatter",
    )(ids, flat_ends, ends, folds, *extra)


def top_kernel(
    sizes, arrived_low, arrived_high, small, dense, labels, w_far, b_first, w_out,
    small_out, fold_low, fold_high,
    vec, gram, feats, preact, pre_grad, pair_grad, w_first, w_sem,
    *, pitch, vec_count,
):
    weights = pltpu.make_async_copy(w_far, w_first, w_sem)
    weights.start()
    feat_count, half, width = arrived_low.shape
    bags = 2 * half
    small_count, batch, _ = small.shape
    shift = batch.bit_length() - 1
    pairs = vec_count * (vec_count - 1) // 2
    scale = width ** (-0.5)
    hidden = w_first.shape[1]
    first_large = 1 + small_count

    def column(row, count=batch, first=0):
        return pl.ds(first * pitch + row, count, stride=pitch)

    for row in range(vec_count, pitch):
        vec[column(row), :] = jnp.zeros((batch, width), F32)
    vec[batch * pitch :, :] = jnp.zeros((vec.shape[0] - batch * pitch, width), F32)
    vec[column(0), :] = dense[...].astype(F32)
    for t in range(small_count):
        vec[column(1 + t), :] = small[t].astype(F32)
    sample = lax.broadcasted_iota(jnp.int32, (batch, bags), 0)
    bag = lax.broadcasted_iota(jnp.int32, (batch, bags), 1)
    for f in range(feat_count):
        hot = jnp.where(((sample * sizes[f]) >> shift) == bag, 1.0, 0.0).astype(BF16)
        vec[column(first_large + f), :] = jnp.dot(
            hot, jnp.concatenate([arrived_low[f], arrived_high[f]], axis=0), preferred_element_type=F32
        )

    together = 8

    def gram_step(s, _):
        base = s * (together * pitch)
        blocks = [
            vec[pl.ds(pl.multiple_of(base + n * pitch, 8), pitch), :].astype(BF16)
            for n in range(together)
        ]
        for n in range(together):
            g = lax.dot_general(
                blocks[n], blocks[n], (((1,), (1,)), ((), ())), preferred_element_type=F32
            )
            gram[pl.ds(pl.multiple_of(base + n * pitch, 8), pitch), 0:pitch] = g * scale
        return 0

    lax.fori_loop(0, batch // together, gram_step, 0)

    part = 64
    lane = lax.broadcasted_iota(jnp.int32, (part, LANES), 1)

    def pack_step(s, _):
        rows = pl.ds(pl.multiple_of(s * part, part), part)
        tile = None
        offset = 0
        for i in range(1, vec_count + 1):
            if i < vec_count:
                piece = gram[pl.ds(s * (part * pitch) + i, part, stride=pitch), :]
                length = i
            else:
                piece = dense[rows, :].astype(F32)
                length = width
            turn = offset % LANES
            number = offset // LANES
            if turn:
                piece = pltpu.roll(piece, turn, 1)
                tile = jnp.where(lane >= turn, piece, tile)
            else:
                tile = piece
            offset += length
            if offset // LANES > number:
                feats[rows, number * LANES : (number + 1) * LANES] = tile.astype(BF16)
                tile = piece
        if offset % LANES:
            number = offset // LANES
            feats[rows, number * LANES : (number + 1) * LANES] = tile.astype(BF16)
        return 0

    lax.fori_loop(0, batch // part, pack_step, 0)

    weights.wait()
    depth = pairs + width
    bulk = depth // LANES * LANES
    wide = 256
    for n in range(0, hidden, wide):
        total = jnp.dot(feats[:, :bulk], w_first[:bulk, n : n + wide], preferred_element_type=F32)
        total = total + jnp.dot(
            feats[:, bulk:depth], w_first[bulk:depth, n : n + wide], preferred_element_type=F32
        )
        preact[:, n : n + wide] = total + b_first[:, n : n + wide]

    def head_step(s, _):
        rows = pl.ds(pl.multiple_of(s * 16, 16), 16)
        v = preact[rows, :]
        squash = jax.nn.sigmoid(v)
        logit = jnp.sum(v * squash * w_out[...], axis=1, keepdims=True)
        logit_grad = jax.nn.sigmoid(logit) - labels[rows, :].astype(F32)
        slope = squash * (1.0 + v * (1.0 - squash))
        pre_grad[rows, :] = (logit_grad * w_out[...] * slope).astype(BF16)
        return 0

    lax.fori_loop(0, batch // 16, head_step, 0)

    bulk = pairs // wide * wide
    for n in range(0, pairs, wide):
        span = min(wide, pairs - n)
        g = lax.dot_general(
            pre_grad[...], w_first[n : n + span, :], (((1,), (1,)), ((), ())),
            preferred_element_type=F32,
        )
        pair_grad[:, n : n + span] = g * scale

    def unpack_step(s, _):
        rows = pl.ds(pl.multiple_of(s * part, part), part)
        offset = 0
        for i in range(pitch):
            where_to = pl.ds(s * (part * pitch) + i, part, stride=pitch)
            if i == 0 or i >= vec_count:
                gram[where_to, :] = jnp.zeros((part, LANES), F32)
                continue
            turn = offset % LANES
            number = offset // LANES
            back = (LANES - turn) % LANES
            piece = pair_grad[rows, number * LANES : (number + 1) * LANES]
            if back:
                piece = pltpu.roll(piece, back, 1)
            if turn + i > LANES:
                more = pair_grad[rows, (number + 1) * LANES : (number + 2) * LANES]
                piece = jnp.where(lane < LANES - turn, piece, pltpu.roll(more, back, 1))
            gram[where_to, :] = jnp.where(lane < i, piece, 0.0)
            offset += i
        return 0

    lax.fori_loop(0, batch // part, unpack_step, 0)

    def grad_step(s, _):
        base = s * (together * pitch)
        found = []
        for n in range(together):
            spot = pl.multiple_of(base + n * pitch, 8)
            lower = gram[pl.ds(spot, pitch), :]
            vectors = vec[pl.ds(spot, pitch), :].astype(BF16)
            found.append((lower, vectors))
        for n in range(together):
            lower, vectors = found[n]
            spot = pl.multiple_of(base + n * pitch, 8)
            both = (lower[:, :pitch] + jnp.transpose(lower)[:pitch, :]).astype(BF16)
            vec[pl.ds(spot, pitch), :] = jnp.dot(both, vectors, preferred_element_type=F32)
        return 0

    lax.fori_loop(0, batch // together, grad_step, 0)

    for t in range(small_count):
        small_out[t] = vec[column(1 + t), :].astype(BF16)
    sample_t = lax.broadcasted_iota(jnp.int32, (bags, batch), 1)
    bag_t = lax.broadcasted_iota(jnp.int32, (bags, batch), 0)
    for f in range(feat_count):
        hot = jnp.where(((sample_t * sizes[f]) >> shift) == bag_t, 1.0, 0.0).astype(BF16)
        grads = vec[column(first_large + f), :].astype(BF16)
        fold = jnp.dot(hot, grads, preferred_element_type=F32).astype(BF16)
        for copy in range(fold_low.shape[0]):
            fold_low[copy, f] = fold[:half]
            fold_high[copy, f] = fold[half:]


def top(sizes, arrived, small, dense, labels, w_first, b_first, w_out, copies):
    feat_count, half, width = arrived[0].shape
    small_count, batch, _ = small.shape
    vec_count = 1 + small_count + feat_count
    pitch = -(-vec_count // 8) * 8
    pairs = vec_count * (vec_count - 1) // 2
    depth = pairs + width
    hidden = w_first.shape[1]

    def up(n):
        return -(-n // LANES) * LANES

    return pl.pallas_call(
        functools.partial(top_kernel, pitch=pitch, vec_count=vec_count),
        out_shape=(
            jax.ShapeDtypeStruct((small_count, batch, width), BF16),
            jax.ShapeDtypeStruct((copies, feat_count, half, width), BF16),
            jax.ShapeDtypeStruct((copies, feat_count, half, width), BF16),
        ),
        in_specs=[whole(pltpu.SMEM)] + [whole()] * 5 + [whole(pl.ANY)] + [whole()] * 2,
        out_specs=(whole(),) * 3,
        scratch_shapes=[
            pltpu.VMEM((batch * pitch + LANES - pitch, width), F32),
            pltpu.VMEM((batch * pitch, LANES), F32),
            pltpu.VMEM((batch, up(depth)), BF16),
            pltpu.VMEM((batch, hidden), F32),
            pltpu.VMEM((batch, hidden), BF16),
            pltpu.VMEM((batch, up(pairs)), F32),
            pltpu.VMEM(w_first.shape, BF16),
            pltpu.SemaphoreType.DMA,
        ],
        compiler_params=pltpu.CompilerParams(vmem_limit_bytes=VMEM_CAP),
        cost_estimate=cost(45),
        name="top",
    )(sizes, *arrived, small, dense, labels, w_first, b_first, w_out)


def step(
    dense, small_ids, labels, small_tables, large_tables,
    batch_sizes, bag_ends, owner_row_index, w_first, b_first, w_out,
):
    groups = 1
    for name in OWNERS:
        groups = groups * lax.axis_size(name)
    copies = lax.axis_size("rep")
    replica = lax.axis_index("rep")
    me = lax.axis_index(ALL)
    small_rows = small_tables.shape[1]
    table = large_tables[0]
    ends = bag_ends[0]
    slots = owner_row_index.shape[2]
    flat_ends = ends.reshape(-1)
    ids = owner_row_index.reshape(-1, 8, slots // 128, 128).transpose(0, 2, 1, 3).reshape(-1)
    first = (replica * groups).astype(jnp.int32).reshape(1)

    ids_sent = lax.all_to_all(small_ids.T[:, None], PLANE, 0, 0, tiled=True)
    sizes = lax.dynamic_slice_in_dim(batch_sizes, me, 1, 1)[:, 0]

    parts = 2
    arrived = []
    for part in range(parts):
        pooled = pool(first, ids, flat_ends, ends, table, groups, slots, part, parts)
        arrived.append(lax.all_to_all(pooled, OWNERS, 0, 0, tiled=True))
    hot = (small_ids.T[:, :, None] == jnp.arange(small_rows, dtype=jnp.int32)).astype(BF16)
    small = jnp.einsum("tbr,tre->tbe", hot, small_tables, preferred_element_type=F32).astype(BF16)

    small_grad, *folded = top(
        sizes, arrived, small, dense, labels[:, None], w_first, b_first[None], w_out[None], copies
    )

    grads = lax.all_to_all(small_grad, PLANE, 0, 0, tiled=True).reshape(-1, LANES)
    owner_hot = (ids_sent.reshape(-1)[:, None] == jnp.arange(small_rows, dtype=jnp.int32)).astype(BF16)
    partial = jnp.einsum("sr,se->re", owner_hot, grads, preferred_element_type=F32)
    found = lax.all_gather(partial.astype(BF16), "x")
    total = found.astype(F32).sum(0)
    table_index = lax.axis_index(PLANE)
    mine_small = lax.dynamic_slice_in_dim(small_tables, table_index, 1, 0)[0]
    new_small = (mine_small.astype(F32) - step_size * total).astype(BF16)
    chips = lax.all_gather(new_small, PLANE[:-1])
    across = lax.ppermute(chips, "core", [(0, 1), (1, 0)])
    shape = (chips.shape[0], 2) + chips.shape[1:]
    here = lax.broadcasted_iota(jnp.int32, shape, 1) == lax.axis_index("core")
    small_new = jnp.where(here, chips[:, None], across[:, None]).reshape(small_tables.shape)

    large_new = None
    for part in range(parts):
        fold = folded[part].reshape((-1,) + folded[part].shape[2:])
        folds = lax.all_to_all(fold, ALL, 0, 0, tiled=True)
        large_new = scatter(ids, flat_ends, ends, folds, large_new, table, slots, part, parts, WAYS)
    return small_new, large_new[None]


def solution(mesh):
    fine = Mesh(mesh.devices.reshape(2, 4, 2, 4, 2), ALL)
    placed = (
        P(ALL, None), P(ALL, None), P(ALL), P(), P(OWNERS, None, None), P(),
        P(OWNERS, None, None), P(OWNERS, None, None), P(), P(), P(),
    )
    return jax.shard_map(
        step, mesh=fine, in_specs=placed, out_specs=(P(), P(OWNERS, None, None)), check_vma=False
    )
```

```python
import functools
import jax
import jax.numpy as jnp
from jax import lax
from jax.experimental import pallas as pl
from jax.experimental.pallas import tpu as pltpu
from jax.sharding import Mesh, PartitionSpec as P

step_size = 32.0
LANES = 128
VMEM_CAP = 67_000_000
F32 = jnp.float32
BF16 = jnp.bfloat16

OWNERS = ("y", "zl", "x", "core")
ALL = ("rep",) + OWNERS
PLANE = ("rep", "y", "zl", "core")


def whole(space=pltpu.VMEM):
    return pl.BlockSpec(memory_space=space)


def bag_mask(ends_row, slots):
    bags = ends_row.shape[1]
    lane = lax.broadcasted_iota(jnp.int32, (1, bags), 1)
    starts = jnp.where(lane == 0, 0, pltpu.roll(ends_row, 1, 1))
    slot = lax.broadcasted_iota(jnp.int32, (slots, bags), 0)
    inside = (slot >= starts) & (slot < ends_row)
    return jnp.where(inside, 1.0, 0.0).astype(BF16)


def cost(micros):
    return pl.CostEstimate(flops=0, bytes_accessed=int(micros * 3.0e6), transcendentals=0)


def slot_base(d, k, slots):
    return (((d >> 3) * (slots // 128) + (k >> 7)) << 10) + ((d & 7) << 7) + (k & 127)


def pool_kernel(first, ids, flat_ends, ends, table, out, wide, rows, *, group, unroll, slots):
    dests, bags, _ = out.shape

    def widen(c, _):
        span = pl.ds(pl.multiple_of(c * 256, 256), 256)
        wide[span, :] = table[span, :].astype(F32)
        return 0

    lax.fori_loop(0, table.shape[0] // 256, widen, 0)
    rows[...] = jnp.zeros(rows.shape, F32)

    def one_group(g, _):
        def one_dest(i, _):
            d = first[0] + g * group + i
            row = i * slots

            def chunk(c, _):
                start = slot_base(d, c * unroll, slots)
                place = row + c * unroll
                for u in range(unroll):
                    rows[pl.ds(place + u, 1), :] = wide[pl.ds(ids[start + u], 1), :]
                return 0

            used = flat_ends[d * bags + bags - 1]
            lax.fori_loop(0, (used + unroll - 1) >> (unroll.bit_length() - 1), chunk, 0)
            return 0

        lax.fori_loop(0, group, one_dest, 0)
        limits = ends[pl.ds(pl.multiple_of(first[0] + g * group, group), group), :]
        for i in range(group):
            mask = bag_mask(limits[i : i + 1], slots)
            taken = rows[i * slots : (i + 1) * slots, :].astype(BF16)
            total = lax.dot_general(
                mask, taken, (((0,), (0,)), ((), ())), preferred_element_type=F32
            )
            out[g * group + i] = total.astype(BF16)
        return 0

    lax.fori_loop(0, dests // group, one_group, 0)


def pool(first, ids, flat_ends, ends, table, dests, slots):
    bags = ends.shape[1]
    group = 8
    return pl.pallas_call(
        functools.partial(pool_kernel, group=group, unroll=32, slots=slots),
        out_shape=jax.ShapeDtypeStruct((dests, bags, LANES), BF16),
        in_specs=[whole(pltpu.SMEM)] * 3 + [whole()] * 2,
        out_specs=whole(),
        scratch_shapes=[
            pltpu.VMEM(table.shape, F32),
            pltpu.VMEM((group * slots, LANES), F32),
        ],
        compiler_params=pltpu.CompilerParams(vmem_limit_bytes=VMEM_CAP),
        cost_estimate=cost(16),
        name="pool",
    )(first, ids, flat_ends, ends, table)


def scatter_kernel(ids, flat_ends, ends, folds, table, out, vals, *accs, group, unroll, slots):
    dests, bags = ends.shape
    ways = len(accs)

    def clear(c, _):
        for acc in accs:
            acc[pl.ds(pl.multiple_of(c * 128, 128), 128), :] = jnp.zeros((128, LANES), F32)
        return 0

    lax.fori_loop(0, out.shape[0] // 128, clear, 0)

    def one_group(g, _):
        limits = ends[pl.ds(pl.multiple_of(g * group, group), group), :]
        for i in range(group):
            mask = bag_mask(limits[i : i + 1], slots)
            vals[i * slots : (i + 1) * slots, :] = jnp.dot(
                mask, folds[g * group + i], preferred_element_type=F32
            )

        def one_dest(i, _):
            d = g * group + i
            row = i * slots

            def chunk(c, _):
                start = slot_base(d, c * unroll, slots)
                place = row + c * unroll
                for v in range(0, unroll, ways):
                    spots = [ids[start + v + w] for w in range(ways)]
                    sums = [
                        accs[w][pl.ds(spots[w], 1), :] + vals[pl.ds(place + v + w, 1), :]
                        for w in range(ways)
                    ]
                    for w in range(ways):
                        accs[w][pl.ds(spots[w], 1), :] = sums[w]
                return 0

            used = flat_ends[d * bags + bags - 1]
            lax.fori_loop(0, (used + unroll - 1) >> (unroll.bit_length() - 1), chunk, 0)
            return 0

        lax.fori_loop(0, group, one_dest, 0)
        return 0

    lax.fori_loop(0, dests // group, one_group, 0)

    def finish(c, _):
        span = pl.ds(pl.multiple_of(c * 128, 128), 128)
        total = accs[0][span, :]
        for acc in accs[1:]:
            total = total + acc[span, :]
        out[span, :] = (table[span, :].astype(F32) - step_size * total).astype(BF16)
        return 0

    lax.fori_loop(0, table.shape[0] // 128, finish, 0)


def scatter(ids, flat_ends, ends, folds, table, slots, ways=8):
    group = 8
    return pl.pallas_call(
        functools.partial(scatter_kernel, group=group, unroll=32, slots=slots),
        out_shape=jax.ShapeDtypeStruct(table.shape, BF16),
        in_specs=[whole(pltpu.SMEM)] * 2 + [whole()] * 3,
        out_specs=whole(),
        scratch_shapes=[pltpu.VMEM((group * slots, LANES), F32)]
        + [pltpu.VMEM(table.shape, F32)] * ways,
        compiler_params=pltpu.CompilerParams(vmem_limit_bytes=VMEM_CAP),
        cost_estimate=cost(28),
        name="scatter",
    )(ids, flat_ends, ends, folds, table)


def top_kernel(
    sizes, arrived, small, dense, labels, w_far, b_first, w_out,
    small_out, fold_out,
    vec, gram, feats, preact, pre_grad, pair_grad, w_first, w_sem,
    *, pitch, vec_count,
):
    weights = pltpu.make_async_copy(w_far, w_first, w_sem)
    weights.start()
    feat_count, bags, width = arrived.shape
    small_count, batch, _ = small.shape
    shift = batch.bit_length() - 1
    pairs = vec_count * (vec_count - 1) // 2
    scale = width ** (-0.5)
    hidden = w_first.shape[1]
    first_large = 1 + small_count

    def column(row, count=batch, first=0):
        return pl.ds(first * pitch + row, count, stride=pitch)

    for row in range(vec_count, pitch):
        vec[column(row), :] = jnp.zeros((batch, width), F32)
    vec[batch * pitch :, :] = jnp.zeros((vec.shape[0] - batch * pitch, width), F32)
    vec[column(0), :] = dense[...].astype(F32)
    for t in range(small_count):
        vec[column(1 + t), :] = small[t].astype(F32)
    sample = lax.broadcasted_iota(jnp.int32, (batch, bags), 0)
    bag = lax.broadcasted_iota(jnp.int32, (batch, bags), 1)
    for f in range(feat_count):
        hot = jnp.where(((sample * sizes[f]) >> shift) == bag, 1.0, 0.0).astype(BF16)
        vec[column(first_large + f), :] = jnp.dot(hot, arrived[f], preferred_element_type=F32)

    together = 8

    def gram_step(s, _):
        base = s * (together * pitch)
        blocks = [
            vec[pl.ds(pl.multiple_of(base + n * pitch, 8), pitch), :].astype(BF16)
            for n in range(together)
        ]
        for n in range(together):
            g = lax.dot_general(
                blocks[n], blocks[n], (((1,), (1,)), ((), ())), preferred_element_type=F32
            )
            gram[pl.ds(pl.multiple_of(base + n * pitch, 8), pitch), 0:pitch] = g * scale
        return 0

    lax.fori_loop(0, batch // together, gram_step, 0)

    part = 64
    lane = lax.broadcasted_iota(jnp.int32, (part, LANES), 1)

    def pack_step(s, _):
        rows = pl.ds(pl.multiple_of(s * part, part), part)
        tile = None
        offset = 0
        for i in range(1, vec_count + 1):
            if i < vec_count:
                piece = gram[pl.ds(s * (part * pitch) + i, part, stride=pitch), :]
                length = i
            else:
                piece = dense[rows, :].astype(F32)
                length = width
            turn = offset % LANES
            number = offset // LANES
            if turn:
                piece = pltpu.roll(piece, turn, 1)
                tile = jnp.where(lane >= turn, piece, tile)
            else:
                tile = piece
            offset += length
            if offset // LANES > number:
                feats[rows, number * LANES : (number + 1) * LANES] = tile.astype(BF16)
                tile = piece
        if offset % LANES:
            number = offset // LANES
            feats[rows, number * LANES : (number + 1) * LANES] = tile.astype(BF16)
        return 0

    lax.fori_loop(0, batch // part, pack_step, 0)

    weights.wait()
    depth = pairs + width
    bulk = depth // LANES * LANES
    wide = 256
    for n in range(0, hidden, wide):
        total = jnp.dot(feats[:, :bulk], w_first[:bulk, n : n + wide], preferred_element_type=F32)
        total = total + jnp.dot(
            feats[:, bulk:depth], w_first[bulk:depth, n : n + wide], preferred_element_type=F32
        )
        preact[:, n : n + wide] = total + b_first[:, n : n + wide]

    def head_step(s, _):
        rows = pl.ds(pl.multiple_of(s * 16, 16), 16)
        v = preact[rows, :]
        squash = jax.nn.sigmoid(v)
        logit = jnp.sum(v * squash * w_out[...], axis=1, keepdims=True)
        logit_grad = jax.nn.sigmoid(logit) - labels[rows, :].astype(F32)
        slope = squash * (1.0 + v * (1.0 - squash))
        pre_grad[rows, :] = (logit_grad * w_out[...] * slope).astype(BF16)
        return 0

    lax.fori_loop(0, batch // 16, head_step, 0)

    bulk = pairs // wide * wide
    for n in range(0, pairs, wide):
        span = min(wide, pairs - n)
        g = lax.dot_general(
            pre_grad[...], w_first[n : n + span, :], (((1,), (1,)), ((), ())),
            preferred_element_type=F32,
        )
        pair_grad[:, n : n + span] = g * scale

    def unpack_step(s, _):
        rows = pl.ds(pl.multiple_of(s * part, part), part)
        offset = 0
        for i in range(pitch):
            where_to = pl.ds(s * (part * pitch) + i, part, stride=pitch)
            if i == 0 or i >= vec_count:
                gram[where_to, :] = jnp.zeros((part, LANES), F32)
                continue
            turn = offset % LANES
            number = offset // LANES
            back = (LANES - turn) % LANES
            piece = pair_grad[rows, number * LANES : (number + 1) * LANES]
            if back:
                piece = pltpu.roll(piece, back, 1)
            if turn + i > LANES:
                more = pair_grad[rows, (number + 1) * LANES : (number + 2) * LANES]
                piece = jnp.where(lane < LANES - turn, piece, pltpu.roll(more, back, 1))
            gram[where_to, :] = jnp.where(lane < i, piece, 0.0)
            offset += i
        return 0

    lax.fori_loop(0, batch // part, unpack_step, 0)

    def grad_step(s, _):
        base = s * (together * pitch)
        found = []
        for n in range(together):
            spot = pl.multiple_of(base + n * pitch, 8)
            lower = gram[pl.ds(spot, pitch), :]
            vectors = vec[pl.ds(spot, pitch), :].astype(BF16)
            found.append((lower, vectors))
        for n in range(together):
            lower, vectors = found[n]
            spot = pl.multiple_of(base + n * pitch, 8)
            both = (lower[:, :pitch] + jnp.transpose(lower)[:pitch, :]).astype(BF16)
            vec[pl.ds(spot, pitch), :] = jnp.dot(both, vectors, preferred_element_type=F32)
        return 0

    lax.fori_loop(0, batch // together, grad_step, 0)

    for t in range(small_count):
        small_out[t] = vec[column(1 + t), :].astype(BF16)
    sample_t = lax.broadcasted_iota(jnp.int32, (bags, batch), 1)
    bag_t = lax.broadcasted_iota(jnp.int32, (bags, batch), 0)
    for f in range(feat_count):
        hot = jnp.where(((sample_t * sizes[f]) >> shift) == bag_t, 1.0, 0.0).astype(BF16)
        grads = vec[column(first_large + f), :].astype(BF16)
        fold = jnp.dot(hot, grads, preferred_element_type=F32).astype(BF16)
        for copy in range(fold_out.shape[0]):
            fold_out[copy, f] = fold


def top(sizes, arrived, small, dense, labels, w_first, b_first, w_out, copies):
    feat_count, bags, width = arrived.shape
    small_count, batch, _ = small.shape
    vec_count = 1 + small_count + feat_count
    pitch = -(-vec_count // 8) * 8
    pairs = vec_count * (vec_count - 1) // 2
    depth = pairs + width
    hidden = w_first.shape[1]

    def up(n):
        return -(-n // LANES) * LANES

    return pl.pallas_call(
        functools.partial(top_kernel, pitch=pitch, vec_count=vec_count),
        out_shape=(
            jax.ShapeDtypeStruct((small_count, batch, width), BF16),
            jax.ShapeDtypeStruct((copies, feat_count, bags, width), BF16),
        ),
        in_specs=[whole(pltpu.SMEM)] + [whole()] * 4 + [whole(pl.ANY)] + [whole()] * 2,
        out_specs=(whole(), whole()),
        scratch_shapes=[
            pltpu.VMEM((batch * pitch + LANES - pitch, width), F32),
            pltpu.VMEM((batch * pitch, LANES), F32),
            pltpu.VMEM((batch, up(depth)), BF16),
            pltpu.VMEM((batch, hidden), F32),
            pltpu.VMEM((batch, hidden), BF16),
            pltpu.VMEM((batch, up(pairs)), F32),
            pltpu.VMEM(w_first.shape, BF16),
            pltpu.SemaphoreType.DMA,
        ],
        compiler_params=pltpu.CompilerParams(vmem_limit_bytes=VMEM_CAP),
        cost_estimate=cost(45),
        name="top",
    )(sizes, arrived, small, dense, labels, w_first, b_first, w_out)


def step(
    dense, small_ids, labels, small_tables, large_tables,
    batch_sizes, bag_ends, owner_row_index, w_first, b_first, w_out,
):
    groups = 1
    for name in OWNERS:
        groups = groups * lax.axis_size(name)
    copies = lax.axis_size("rep")
    replica = lax.axis_index("rep")
    me = lax.axis_index(ALL)
    small_rows = small_tables.shape[1]
    table = large_tables[0]
    ends = bag_ends[0]
    slots = owner_row_index.shape[2]
    flat_ends = ends.reshape(-1)
    ids = owner_row_index.reshape(-1, 8, slots // 128, 128).transpose(0, 2, 1, 3).reshape(-1)
    first = (replica * groups).astype(jnp.int32).reshape(1)

    ids_sent = lax.all_gather(small_ids.T, PLANE)
    ids_sent = lax.dynamic_index_in_dim(ids_sent, lax.axis_index(PLANE), 1, False)
    sizes = lax.dynamic_slice_in_dim(batch_sizes, me, 1, 1)[:, 0]

    pooled = pool(first, ids, flat_ends, ends, table, groups, slots)
    arrived = lax.all_to_all(pooled, OWNERS, 0, 0, tiled=True)
    hot = (small_ids.T[:, :, None] == jnp.arange(small_rows, dtype=jnp.int32)).astype(BF16)
    small = jnp.einsum("tbr,tre->tbe", hot, small_tables, preferred_element_type=F32).astype(BF16)

    small_grad, folded = top(
        sizes, arrived, small, dense, labels[:, None], w_first, b_first[None], w_out[None], copies
    )

    grads = lax.all_to_all(small_grad, PLANE, 0, 0, tiled=True).reshape(-1, LANES)
    owner_hot = (ids_sent.reshape(-1)[:, None] == jnp.arange(small_rows, dtype=jnp.int32)).astype(BF16)
    partial = jnp.einsum("sr,se->re", owner_hot, grads, preferred_element_type=F32)
    found = lax.all_gather(partial.astype(BF16), "x")
    total = found.astype(F32).sum(0)
    table_index = lax.axis_index(PLANE)
    mine_small = lax.dynamic_slice_in_dim(small_tables, table_index, 1, 0)[0]
    new_small = (mine_small.astype(F32) - step_size * total).astype(BF16)
    small_new = lax.all_gather(new_small, PLANE)

    folds = lax.all_to_all(folded.reshape((-1,) + folded.shape[2:]), ALL, 0, 0, tiled=True)
    large_new = scatter(ids, flat_ends, ends, folds, table, slots)
    return small_new, large_new[None]


def solution(mesh):
    fine = Mesh(mesh.devices.reshape(2, 4, 2, 4, 2), ALL)
    placed = (
        P(ALL, None), P(ALL, None), P(ALL), P(), P(OWNERS, None, None), P(),
        P(OWNERS, None, None), P(OWNERS, None, None), P(), P(), P(),
    )
    return jax.shard_map(
        step, mesh=fine, in_specs=placed, out_specs=(P(), P(OWNERS, None, None)), check_vma=False
    )
```

```python
import functools
import jax
import jax.numpy as jnp
from jax import lax
from jax.experimental import pallas as pl
from jax.experimental.pallas import tpu as pltpu
from jax.sharding import Mesh, PartitionSpec as P

step_size = 32.0
LANES = 128
VMEM_CAP = 67_000_000
F32 = jnp.float32
BF16 = jnp.bfloat16

OWNERS = ("y", "zl", "x", "core")
ALL = ("rep",) + OWNERS
PLANE = ("rep", "y", "zl", "core")


def whole(space=pltpu.VMEM):
    return pl.BlockSpec(memory_space=space)


def bag_mask(ends_row, slots):
    bags = ends_row.shape[1]
    lane = lax.broadcasted_iota(jnp.int32, (1, bags), 1)
    starts = jnp.where(lane == 0, 0, pltpu.roll(ends_row, 1, 1))
    slot = lax.broadcasted_iota(jnp.int32, (slots, bags), 0)
    inside = (slot >= starts) & (slot < ends_row)
    return jnp.where(inside, 1.0, 0.0).astype(BF16)


def cost(micros):
    return pl.CostEstimate(flops=0, bytes_accessed=int(micros * 3.0e6), transcendentals=0)


def slot_base(d, k, slots):
    return (((d >> 3) * (slots // 128) + (k >> 7)) << 10) + ((d & 7) << 7) + (k & 127)


def pool_kernel(
    ids, ends, table, arrived, wide, rows, pooled, send_sem, recv_sem, self_sem, *, group, unroll, slots
):
    dests = arrived.shape[0]
    groups = dests // group
    row_index = lax.axis_index("y") * lax.axis_size("zl") + lax.axis_index("zl")
    mine = row_index * group + lax.axis_index("x") * lax.axis_size("core") + lax.axis_index("core")
    first = lax.axis_index("rep") * dests

    def place(g, i):
        return {
            "y": g // lax.axis_size("zl"),
            "zl": lax.rem(g, lax.axis_size("zl")),
            "x": i // lax.axis_size("core"),
            "core": i % lax.axis_size("core"),
        }

    barrier = pltpu.get_barrier_semaphore()

    def greet(g, _):
        for i in range(group):

            @pl.when(g * group + i != mine)
            def _():
                pl.semaphore_signal(
                    barrier, 1, device_id=place(g, i), device_id_type=pl.DeviceIdType.MESH
                )

        return 0

    lax.fori_loop(0, groups, greet, 0)

    def widen(c, _):
        span = pl.ds(pl.multiple_of(c * 256, 256), 256)
        wide[span, :] = table[span, :].astype(F32)
        return 0

    lax.fori_loop(0, table.shape[0] // 256, widen, 0)
    pl.semaphore_wait(barrier, dests - 1)

    def turn(step):
        return lax.rem(row_index + step, groups)

    def send(step):
        g = turn(step)
        for i in range(group):
            d = g * group + i

            @pl.when(d != mine)
            def _():
                pltpu.make_async_remote_copy(
                    src_ref=pooled.at[d],
                    dst_ref=arrived.at[mine],
                    send_sem=send_sem,
                    recv_sem=recv_sem,
                    device_id=place(g, i),
                    device_id_type=pl.DeviceIdType.MESH,
                ).start()

    def one_group(step, _):
        g = turn(step)

        def one_dest(i, _):
            d = first + g * group + i
            row = i * slots

            def chunk(c, _):
                start = slot_base(d, c * unroll, slots)
                spot = row + c * unroll
                for u in range(unroll):
                    rows[pl.ds(spot + u, 1), :] = wide[pl.ds(ids[start + u], 1), :]
                return 0

            lax.fori_loop(0, slots // unroll, chunk, 0)
            return 0

        lax.fori_loop(0, group, one_dest, 0)

        @pl.when(step > 0)
        def _():
            send(step - 1)

        limits = ends[pl.ds(pl.multiple_of(first + g * group, group), group), :]
        for i in range(group):
            mask = bag_mask(limits[i : i + 1], slots)
            taken = rows[i * slots : (i + 1) * slots, :].astype(BF16)
            total = lax.dot_general(
                mask, taken, (((0,), (0,)), ((), ())), preferred_element_type=F32
            )
            pooled[g * group + i] = total.astype(BF16)
        return 0

    lax.fori_loop(0, groups, one_group, 0)
    own = pltpu.make_async_copy(pooled.at[mine], arrived.at[mine], self_sem)
    own.start()
    send(groups - 1)
    own.wait()
    whole_span = pl.ds(0, dests - 1)
    every = pltpu.make_async_remote_copy(
        src_ref=pooled.at[whole_span],
        dst_ref=arrived.at[whole_span],
        send_sem=send_sem,
        recv_sem=recv_sem,
        device_id=place(lax.rem(row_index + 1, groups), 0),
        device_id_type=pl.DeviceIdType.MESH,
    )
    every.wait_send()
    every.wait_recv()


def pool_and_send(ids, ends, table, dests, slots):
    bags = ends.shape[1]
    group = 8
    return pl.pallas_call(
        functools.partial(pool_kernel, group=group, unroll=64, slots=slots),
        out_shape=jax.ShapeDtypeStruct((dests, bags, LANES), BF16),
        in_specs=[whole(pltpu.SMEM)] + [whole()] * 2,
        out_specs=whole(pl.ANY),
        scratch_shapes=[
            pltpu.VMEM(table.shape, F32),
            pltpu.VMEM((group * slots, LANES), F32),
            pltpu.VMEM((dests, bags, LANES), BF16),
            pltpu.SemaphoreType.DMA,
            pltpu.SemaphoreType.DMA,
            pltpu.SemaphoreType.DMA,
        ],
        compiler_params=pltpu.CompilerParams(
            vmem_limit_bytes=VMEM_CAP, collective_id=0, has_side_effects=True
        ),
        cost_estimate=cost(32),
        name="pool",
    )(ids, ends, table)


def scatter_kernel(ids, flat_ends, ends, folds, table, out, vals, *accs, group, unroll, slots):
    dests, bags = ends.shape
    ways = len(accs)

    def clear(c, _):
        for acc in accs:
            acc[pl.ds(pl.multiple_of(c * 128, 128), 128), :] = jnp.zeros((128, LANES), F32)
        return 0

    lax.fori_loop(0, out.shape[0] // 128, clear, 0)

    def one_group(g, _):
        limits = ends[pl.ds(pl.multiple_of(g * group, group), group), :]
        for i in range(group):
            mask = bag_mask(limits[i : i + 1], slots)
            vals[i * slots : (i + 1) * slots, :] = jnp.dot(
                mask, folds[g * group + i], preferred_element_type=F32
            )

        def one_dest(i, _):
            d = g * group + i
            row = i * slots

            def chunk(c, _):
                start = slot_base(d, c * unroll, slots)
                place = row + c * unroll
                for v in range(0, unroll, ways):
                    spots = [ids[start + v + w] for w in range(ways)]
                    sums = [
                        accs[w][pl.ds(spots[w], 1), :] + vals[pl.ds(place + v + w, 1), :]
                        for w in range(ways)
                    ]
                    for w in range(ways):
                        accs[w][pl.ds(spots[w], 1), :] = sums[w]
                return 0

            used = flat_ends[d * bags + bags - 1]
            lax.fori_loop(0, (used + unroll - 1) >> (unroll.bit_length() - 1), chunk, 0)
            return 0

        lax.fori_loop(0, group, one_dest, 0)
        return 0

    lax.fori_loop(0, dests // group, one_group, 0)

    def finish(c, _):
        span = pl.ds(pl.multiple_of(c * 128, 128), 128)
        total = accs[0][span, :]
        for acc in accs[1:]:
            total = total + acc[span, :]
        out[span, :] = (table[span, :].astype(F32) - step_size * total).astype(BF16)
        return 0

    lax.fori_loop(0, table.shape[0] // 128, finish, 0)


def scatter(ids, flat_ends, ends, folds, table, slots, ways=8):
    group = 8
    return pl.pallas_call(
        functools.partial(scatter_kernel, group=group, unroll=32, slots=slots),
        out_shape=jax.ShapeDtypeStruct(table.shape, BF16),
        in_specs=[whole(pltpu.SMEM)] * 2 + [whole()] * 3,
        out_specs=whole(),
        scratch_shapes=[pltpu.VMEM((group * slots, LANES), F32)]
        + [pltpu.VMEM(table.shape, F32)] * ways,
        compiler_params=pltpu.CompilerParams(vmem_limit_bytes=VMEM_CAP),
        cost_estimate=cost(28),
        name="scatter",
    )(ids, flat_ends, ends, folds, table)


def top_kernel(
    sizes, arrived, small, dense, labels, w_far, b_first, w_out,
    small_out, fold_out,
    vec, gram, feats, preact, pre_grad, pair_grad, w_first, w_sem,
    *, pitch, vec_count,
):
    weights = pltpu.make_async_copy(w_far, w_first, w_sem)
    weights.start()
    feat_count, bags, width = arrived.shape
    small_count, batch, _ = small.shape
    shift = batch.bit_length() - 1
    pairs = vec_count * (vec_count - 1) // 2
    scale = width ** (-0.5)
    hidden = w_first.shape[1]
    first_large = 1 + small_count

    def column(row, count=batch, first=0):
        return pl.ds(first * pitch + row, count, stride=pitch)

    for row in range(vec_count, pitch):
        vec[column(row), :] = jnp.zeros((batch, width), F32)
    vec[batch * pitch :, :] = jnp.zeros((vec.shape[0] - batch * pitch, width), F32)
    vec[column(0), :] = dense[...].astype(F32)
    for t in range(small_count):
        vec[column(1 + t), :] = small[t].astype(F32)
    sample = lax.broadcasted_iota(jnp.int32, (batch, bags), 0)
    bag = lax.broadcasted_iota(jnp.int32, (batch, bags), 1)
    for f in range(feat_count):
        hot = jnp.where(((sample * sizes[f]) >> shift) == bag, 1.0, 0.0).astype(BF16)
        vec[column(first_large + f), :] = jnp.dot(hot, arrived[f], preferred_element_type=F32)

    together = 8

    def gram_step(s, _):
        base = s * (together * pitch)
        blocks = [
            vec[pl.ds(pl.multiple_of(base + n * pitch, 8), pitch), :].astype(BF16)
            for n in range(together)
        ]
        for n in range(together):
            g = lax.dot_general(
                blocks[n], blocks[n], (((1,), (1,)), ((), ())), preferred_element_type=F32
            )
            gram[pl.ds(pl.multiple_of(base + n * pitch, 8), pitch), 0:pitch] = g * scale
        return 0

    lax.fori_loop(0, batch // together, gram_step, 0)

    part = 64
    lane = lax.broadcasted_iota(jnp.int32, (part, LANES), 1)

    def pack_step(s, _):
        rows = pl.ds(pl.multiple_of(s * part, part), part)
        tile = None
        offset = 0
        for i in range(1, vec_count + 1):
            if i < vec_count:
                piece = gram[pl.ds(s * (part * pitch) + i, part, stride=pitch), :]
                length = i
            else:
                piece = dense[rows, :].astype(F32)
                length = width
            turn = offset % LANES
            number = offset // LANES
            if turn:
                piece = pltpu.roll(piece, turn, 1)
                tile = jnp.where(lane >= turn, piece, tile)
            else:
                tile = piece
            offset += length
            if offset // LANES > number:
                feats[rows, number * LANES : (number + 1) * LANES] = tile.astype(BF16)
                tile = piece
        if offset % LANES:
            number = offset // LANES
            feats[rows, number * LANES : (number + 1) * LANES] = tile.astype(BF16)
        return 0

    lax.fori_loop(0, batch // part, pack_step, 0)

    weights.wait()
    depth = pairs + width
    bulk = depth // LANES * LANES
    wide = 256
    for n in range(0, hidden, wide):
        total = jnp.dot(feats[:, :bulk], w_first[:bulk, n : n + wide], preferred_element_type=F32)
        total = total + jnp.dot(
            feats[:, bulk:depth], w_first[bulk:depth, n : n + wide], preferred_element_type=F32
        )
        preact[:, n : n + wide] = total + b_first[:, n : n + wide]

    def head_step(s, _):
        rows = pl.ds(pl.multiple_of(s * 16, 16), 16)
        v = preact[rows, :]
        squash = jax.nn.sigmoid(v)
        logit = jnp.sum(v * squash * w_out[...], axis=1, keepdims=True)
        logit_grad = jax.nn.sigmoid(logit) - labels[rows, :].astype(F32)
        slope = squash * (1.0 + v * (1.0 - squash))
        pre_grad[rows, :] = (logit_grad * w_out[...] * slope).astype(BF16)
        return 0

    lax.fori_loop(0, batch // 16, head_step, 0)

    bulk = pairs // wide * wide
    for n in range(0, pairs, wide):
        span = min(wide, pairs - n)
        g = lax.dot_general(
            pre_grad[...], w_first[n : n + span, :], (((1,), (1,)), ((), ())),
            preferred_element_type=F32,
        )
        pair_grad[:, n : n + span] = g * scale

    def unpack_step(s, _):
        rows = pl.ds(pl.multiple_of(s * part, part), part)
        offset = 0
        for i in range(pitch):
            where_to = pl.ds(s * (part * pitch) + i, part, stride=pitch)
            if i == 0 or i >= vec_count:
                gram[where_to, :] = jnp.zeros((part, LANES), F32)
                continue
            turn = offset % LANES
            number = offset // LANES
            back = (LANES - turn) % LANES
            piece = pair_grad[rows, number * LANES : (number + 1) * LANES]
            if back:
                piece = pltpu.roll(piece, back, 1)
            if turn + i > LANES:
                more = pair_grad[rows, (number + 1) * LANES : (number + 2) * LANES]
                piece = jnp.where(lane < LANES - turn, piece, pltpu.roll(more, back, 1))
            gram[where_to, :] = jnp.where(lane < i, piece, 0.0)
            offset += i
        return 0

    lax.fori_loop(0, batch // part, unpack_step, 0)

    def grad_step(s, _):
        base = s * (together * pitch)
        found = []
        for n in range(together):
            spot = pl.multiple_of(base + n * pitch, 8)
            lower = gram[pl.ds(spot, pitch), :]
            vectors = vec[pl.ds(spot, pitch), :].astype(BF16)
            found.append((lower, vectors))
        for n in range(together):
            lower, vectors = found[n]
            spot = pl.multiple_of(base + n * pitch, 8)
            both = (lower[:, :pitch] + jnp.transpose(lower)[:pitch, :]).astype(BF16)
            vec[pl.ds(spot, pitch), :] = jnp.dot(both, vectors, preferred_element_type=F32)
        return 0

    lax.fori_loop(0, batch // together, grad_step, 0)

    for t in range(small_count):
        small_out[t] = vec[column(1 + t), :].astype(BF16)
    sample_t = lax.broadcasted_iota(jnp.int32, (bags, batch), 1)
    bag_t = lax.broadcasted_iota(jnp.int32, (bags, batch), 0)
    for f in range(feat_count):
        hot = jnp.where(((sample_t * sizes[f]) >> shift) == bag_t, 1.0, 0.0).astype(BF16)
        grads = vec[column(first_large + f), :].astype(BF16)
        fold = jnp.dot(hot, grads, preferred_element_type=F32).astype(BF16)
        for copy in range(fold_out.shape[0]):
            fold_out[copy, f] = fold


def top(sizes, arrived, small, dense, labels, w_first, b_first, w_out, copies):
    feat_count, bags, width = arrived.shape
    small_count, batch, _ = small.shape
    vec_count = 1 + small_count + feat_count
    pitch = -(-vec_count // 8) * 8
    pairs = vec_count * (vec_count - 1) // 2
    depth = pairs + width
    hidden = w_first.shape[1]

    def up(n):
        return -(-n // LANES) * LANES

    return pl.pallas_call(
        functools.partial(top_kernel, pitch=pitch, vec_count=vec_count),
        out_shape=(
            jax.ShapeDtypeStruct((small_count, batch, width), BF16),
            jax.ShapeDtypeStruct((copies, feat_count, bags, width), BF16),
        ),
        in_specs=[whole(pltpu.SMEM)] + [whole()] * 4 + [whole(pl.ANY)] + [whole()] * 2,
        out_specs=(whole(), whole()),
        scratch_shapes=[
            pltpu.VMEM((batch * pitch + LANES - pitch, width), F32),
            pltpu.VMEM((batch * pitch, LANES), F32),
            pltpu.VMEM((batch, up(depth)), BF16),
            pltpu.VMEM((batch, hidden), F32),
            pltpu.VMEM((batch, hidden), BF16),
            pltpu.VMEM((batch, up(pairs)), F32),
            pltpu.VMEM(w_first.shape, BF16),
            pltpu.SemaphoreType.DMA,
        ],
        compiler_params=pltpu.CompilerParams(vmem_limit_bytes=VMEM_CAP),
        cost_estimate=cost(45),
        name="top",
    )(sizes, arrived, small, dense, labels, w_first, b_first, w_out)


def step(
    dense, small_ids, labels, small_tables, large_tables,
    batch_sizes, bag_ends, owner_row_index, w_first, b_first, w_out,
):
    groups = 1
    for name in OWNERS:
        groups = groups * lax.axis_size(name)
    copies = lax.axis_size("rep")
    me = lax.axis_index(ALL)
    small_rows = small_tables.shape[1]
    table = large_tables[0]
    ends = bag_ends[0]
    slots = owner_row_index.shape[2]
    flat_ends = ends.reshape(-1)
    ids = owner_row_index.reshape(-1, 8, slots // 128, 128).transpose(0, 2, 1, 3).reshape(-1)

    sizes = lax.dynamic_slice_in_dim(batch_sizes, me, 1, 1)[:, 0]

    arrived = pool_and_send(ids, ends, table, groups, slots)
    later_ids, arrived = lax.optimization_barrier((small_ids, arrived))
    ids_sent = lax.all_gather(later_ids.T, PLANE)
    ids_sent = lax.dynamic_index_in_dim(ids_sent, lax.axis_index(PLANE), 1, False)
    hot = (small_ids.T[:, :, None] == jnp.arange(small_rows, dtype=jnp.int32)).astype(BF16)
    small = jnp.einsum("tbr,tre->tbe", hot, small_tables, preferred_element_type=F32).astype(BF16)

    small_grad, folded = top(
        sizes, arrived, small, dense, labels[:, None], w_first, b_first[None], w_out[None], copies
    )

    grads = lax.all_to_all(small_grad, PLANE, 0, 0, tiled=True).reshape(-1, LANES)
    owner_hot = (ids_sent.reshape(-1)[:, None] == jnp.arange(small_rows, dtype=jnp.int32)).astype(BF16)
    partial = jnp.einsum("sr,se->re", owner_hot, grads, preferred_element_type=F32)
    found = lax.all_gather(partial.astype(BF16), "x")
    total = found.astype(F32).sum(0)
    table_index = lax.axis_index(PLANE)
    mine_small = lax.dynamic_slice_in_dim(small_tables, table_index, 1, 0)[0]
    new_small = (mine_small.astype(F32) - step_size * total).astype(BF16)
    small_new = lax.all_gather(new_small, PLANE)

    folds = lax.all_to_all(folded.reshape((-1,) + folded.shape[2:]), ALL, 0, 0, tiled=True)
    large_new = scatter(ids, flat_ends, ends, folds, table, slots)
    return small_new, large_new[None]


def solution(mesh):
    fine = Mesh(mesh.devices.reshape(2, 4, 2, 4, 2), ALL)
    placed = (
        P(ALL, None), P(ALL, None), P(ALL), P(), P(OWNERS, None, None), P(),
        P(OWNERS, None, None), P(OWNERS, None, None), P(), P(), P(),
    )
    return jax.shard_map(
        step, mesh=fine, in_specs=placed, out_specs=(P(), P(OWNERS, None, None)), check_vma=False
    )
```

```python
import functools
import jax
import jax.numpy as jnp
from jax import lax
from jax.experimental import pallas as pl
from jax.experimental.pallas import tpu as pltpu
from jax.sharding import Mesh, PartitionSpec as P

step_size = 32.0
LANES = 128
VMEM_CAP = 67_000_000
F32 = jnp.float32
BF16 = jnp.bfloat16

OWNERS = ("y", "zl", "x", "core")
ALL = ("rep",) + OWNERS
PLANE = ("rep", "y", "zl", "core")


def whole(space=pltpu.VMEM):
    return pl.BlockSpec(memory_space=space)


def bag_mask(ends_row, slots):
    bags = ends_row.shape[1]
    lane = lax.broadcasted_iota(jnp.int32, (1, bags), 1)
    starts = jnp.where(lane == 0, 0, pltpu.roll(ends_row, 1, 1))
    slot = lax.broadcasted_iota(jnp.int32, (slots, bags), 0)
    inside = (slot >= starts) & (slot < ends_row)
    return jnp.where(inside, 1.0, 0.0).astype(BF16)


def cost(micros):
    return pl.CostEstimate(flops=0, bytes_accessed=int(micros * 3.0e6), transcendentals=0)


def slot_base(d, k, slots):
    return (((d >> 3) * (slots // 128) + (k >> 7)) << 10) + ((d & 7) << 7) + (k & 127)


def pool_kernel(
    ids, ends, small_ids, table, small_far, arrived, small,
    wide, rows, pooled, small_tables, send_sem, recv_sem, self_sem, small_sem, *, group, unroll, slots
):
    dests = arrived.shape[0]
    groups = dests // group
    row_index = lax.axis_index("y") * lax.axis_size("zl") + lax.axis_index("zl")
    mine = row_index * group + lax.axis_index("x") * lax.axis_size("core") + lax.axis_index("core")
    first = lax.axis_index("rep") * dests

    def place(g, i):
        return {
            "y": g // lax.axis_size("zl"),
            "zl": lax.rem(g, lax.axis_size("zl")),
            "x": i // lax.axis_size("core"),
            "core": i % lax.axis_size("core"),
        }

    tables = pltpu.make_async_copy(small_far, small_tables, small_sem)
    tables.start()
    barrier = pltpu.get_barrier_semaphore()

    def greet(g, _):
        for i in range(group):

            @pl.when(g * group + i != mine)
            def _():
                pl.semaphore_signal(
                    barrier, 1, device_id=place(g, i), device_id_type=pl.DeviceIdType.MESH
                )

        return 0

    lax.fori_loop(0, groups, greet, 0)

    def widen(c, _):
        span = pl.ds(pl.multiple_of(c * 256, 256), 256)
        wide[span, :] = table[span, :].astype(F32)
        return 0

    lax.fori_loop(0, table.shape[0] // 256, widen, 0)
    pl.semaphore_wait(barrier, dests - 1)

    half = groups // 2

    def turn(step):
        y = lax.rem(lax.axis_index("y") + 2 + 3 * step, half)
        return y * 2 + lax.rem(lax.axis_index("zl") + 1 + step // half, 2)

    def send(step):
        g = turn(step)
        for i in range(group):
            d = g * group + i

            @pl.when(d != mine)
            def _():
                pltpu.make_async_remote_copy(
                    src_ref=pooled.at[d],
                    dst_ref=arrived.at[mine],
                    send_sem=send_sem,
                    recv_sem=recv_sem,
                    device_id=place(g, i),
                    device_id_type=pl.DeviceIdType.MESH,
                ).start()

    def one_group(step, _):
        g = turn(step)

        def one_dest(i, _):
            d = first + g * group + i
            row = i * slots

            def chunk(c, _):
                start = slot_base(d, c * unroll, slots)
                spot = row + c * unroll
                for u in range(unroll):
                    rows[pl.ds(spot + u, 1), :] = wide[pl.ds(ids[start + u], 1), :]
                return 0

            lax.fori_loop(0, slots // unroll, chunk, 0)
            return 0

        lax.fori_loop(0, group, one_dest, 0)

        @pl.when(step > 0)
        def _():
            send(step - 1)

        limits = ends[pl.ds(pl.multiple_of(first + g * group, group), group), :]
        for i in range(group):
            mask = bag_mask(limits[i : i + 1], slots)
            taken = rows[i * slots : (i + 1) * slots, :].astype(BF16)
            total = lax.dot_general(
                mask, taken, (((0,), (0,)), ((), ())), preferred_element_type=F32
            )
            pooled[g * group + i] = total.astype(BF16)
        return 0

    lax.fori_loop(0, groups, one_group, 0)
    own = pltpu.make_async_copy(pooled.at[mine], arrived.at[mine], self_sem)
    own.start()
    send(groups - 1)
    tables.wait()
    count, small_rows, _ = small_tables.shape
    batch = small_ids.shape[1]
    columns = jnp.transpose(small_ids[...].astype(F32))
    row = lax.broadcasted_iota(jnp.int32, (batch, small_rows), 1).astype(F32)
    for t in range(count):
        hot = jnp.where(columns[:, t : t + 1] == row, 1.0, 0.0).astype(BF16)
        small[t] = jnp.dot(hot, small_tables[t], preferred_element_type=F32).astype(BF16)
    own.wait()
    whole_span = pl.ds(0, dests - 1)
    every = pltpu.make_async_remote_copy(
        src_ref=pooled.at[whole_span],
        dst_ref=arrived.at[whole_span],
        send_sem=send_sem,
        recv_sem=recv_sem,
        device_id=place(lax.rem(row_index + 1, groups), 0),
        device_id_type=pl.DeviceIdType.MESH,
    )
    every.wait_send()
    every.wait_recv()


def pool_and_send(ids, ends, small_ids, table, small_tables, dests, slots):
    bags = ends.shape[1]
    group = 8
    return pl.pallas_call(
        functools.partial(pool_kernel, group=group, unroll=64, slots=slots),
        out_shape=(
            jax.ShapeDtypeStruct((dests, bags, LANES), BF16),
            jax.ShapeDtypeStruct(small_ids.shape + (LANES,), BF16),
        ),
        in_specs=[whole(pltpu.SMEM)] + [whole()] * 3 + [whole(pl.ANY)],
        out_specs=(whole(pl.ANY), whole()),
        scratch_shapes=[
            pltpu.VMEM(table.shape, F32),
            pltpu.VMEM((group * slots, LANES), F32),
            pltpu.VMEM((dests, bags, LANES), BF16),
            pltpu.VMEM(small_tables.shape, BF16),
            pltpu.SemaphoreType.DMA,
            pltpu.SemaphoreType.DMA,
            pltpu.SemaphoreType.DMA,
            pltpu.SemaphoreType.DMA,
        ],
        compiler_params=pltpu.CompilerParams(
            vmem_limit_bytes=VMEM_CAP, collective_id=0, has_side_effects=True
        ),
        cost_estimate=cost(32),
        name="pool",
    )(ids, ends, small_ids, table, small_tables)


def scatter_kernel(ids, flat_ends, ends, folds, table, out, vals, *accs, group, unroll, slots):
    dests, bags = ends.shape
    ways = len(accs)

    def clear(c, _):
        for acc in accs:
            acc[pl.ds(pl.multiple_of(c * 128, 128), 128), :] = jnp.zeros((128, LANES), F32)
        return 0

    lax.fori_loop(0, out.shape[0] // 128, clear, 0)

    def one_group(g, _):
        limits = ends[pl.ds(pl.multiple_of(g * group, group), group), :]
        for i in range(group):
            mask = bag_mask(limits[i : i + 1], slots)
            vals[i * slots : (i + 1) * slots, :] = jnp.dot(
                mask, folds[g * group + i], preferred_element_type=F32
            )

        def one_dest(i, _):
            d = g * group + i
            row = i * slots

            def chunk(c, _):
                start = slot_base(d, c * unroll, slots)
                place = row + c * unroll
                for v in range(0, unroll, ways):
                    spots = [ids[start + v + w] for w in range(ways)]
                    sums = [
                        accs[w][pl.ds(spots[w], 1), :] + vals[pl.ds(place + v + w, 1), :]
                        for w in range(ways)
                    ]
                    for w in range(ways):
                        accs[w][pl.ds(spots[w], 1), :] = sums[w]
                return 0

            used = flat_ends[d * bags + bags - 1]
            lax.fori_loop(0, (used + unroll - 1) >> (unroll.bit_length() - 1), chunk, 0)
            return 0

        lax.fori_loop(0, group, one_dest, 0)
        return 0

    lax.fori_loop(0, dests // group, one_group, 0)

    def finish(c, _):
        span = pl.ds(pl.multiple_of(c * 128, 128), 128)
        total = accs[0][span, :]
        for acc in accs[1:]:
            total = total + acc[span, :]
        out[span, :] = (table[span, :].astype(F32) - step_size * total).astype(BF16)
        return 0

    lax.fori_loop(0, table.shape[0] // 128, finish, 0)


def scatter(ids, flat_ends, ends, folds, table, slots, ways=8):
    group = 8
    return pl.pallas_call(
        functools.partial(scatter_kernel, group=group, unroll=32, slots=slots),
        out_shape=jax.ShapeDtypeStruct(table.shape, BF16),
        in_specs=[whole(pltpu.SMEM)] * 2 + [whole()] * 3,
        out_specs=whole(),
        scratch_shapes=[pltpu.VMEM((group * slots, LANES), F32)]
        + [pltpu.VMEM(table.shape, F32)] * ways,
        compiler_params=pltpu.CompilerParams(vmem_limit_bytes=VMEM_CAP),
        cost_estimate=cost(28),
        name="scatter",
    )(ids, flat_ends, ends, folds, table)


def top_kernel(
    sizes, arrived, small, dense, labels, w_far, b_first, w_out,
    small_out, fold_out,
    vec, gram, feats, preact, pre_grad, pair_grad, w_first, w_sem,
    *, pitch, vec_count,
):
    weights = pltpu.make_async_copy(w_far, w_first, w_sem)
    weights.start()
    feat_count, bags, width = arrived.shape
    small_count, batch, _ = small.shape
    shift = batch.bit_length() - 1
    pairs = vec_count * (vec_count - 1) // 2
    scale = width ** (-0.5)
    hidden = w_first.shape[1]
    first_large = 1 + small_count

    def column(row, count=batch, first=0):
        return pl.ds(first * pitch + row, count, stride=pitch)

    for row in range(vec_count, pitch):
        vec[column(row), :] = jnp.zeros((batch, width), F32)
    vec[batch * pitch :, :] = jnp.zeros((vec.shape[0] - batch * pitch, width), F32)
    vec[column(0), :] = dense[...].astype(F32)
    for t in range(small_count):
        vec[column(1 + t), :] = small[t].astype(F32)
    sample = lax.broadcasted_iota(jnp.int32, (batch, bags), 0)
    bag = lax.broadcasted_iota(jnp.int32, (batch, bags), 1)
    for f in range(feat_count):
        hot = jnp.where(((sample * sizes[f]) >> shift) == bag, 1.0, 0.0).astype(BF16)
        vec[column(first_large + f), :] = jnp.dot(hot, arrived[f], preferred_element_type=F32)

    together = 8

    def gram_step(s, _):
        base = s * (together * pitch)
        blocks = [
            vec[pl.ds(pl.multiple_of(base + n * pitch, 8), pitch), :].astype(BF16)
            for n in range(together)
        ]
        for n in range(together):
            g = lax.dot_general(
                blocks[n], blocks[n], (((1,), (1,)), ((), ())), preferred_element_type=F32
            )
            gram[pl.ds(pl.multiple_of(base + n * pitch, 8), pitch), 0:pitch] = g * scale
        return 0

    lax.fori_loop(0, batch // together, gram_step, 0)

    part = 64
    lane = lax.broadcasted_iota(jnp.int32, (part, LANES), 1)

    def pack_step(s, _):
        rows = pl.ds(pl.multiple_of(s * part, part), part)
        tile = None
        offset = 0
        for i in range(1, vec_count + 1):
            if i < vec_count:
                piece = gram[pl.ds(s * (part * pitch) + i, part, stride=pitch), :]
                length = i
            else:
                piece = dense[rows, :].astype(F32)
                length = width
            turn = offset % LANES
            number = offset // LANES
            if turn:
                piece = pltpu.roll(piece, turn, 1)
                tile = jnp.where(lane >= turn, piece, tile)
            else:
                tile = piece
            offset += length
            if offset // LANES > number:
                feats[rows, number * LANES : (number + 1) * LANES] = tile.astype(BF16)
                tile = piece
        if offset % LANES:
            number = offset // LANES
            feats[rows, number * LANES : (number + 1) * LANES] = tile.astype(BF16)
        return 0

    lax.fori_loop(0, batch // part, pack_step, 0)

    weights.wait()
    depth = pairs + width
    bulk = depth // LANES * LANES
    wide = 256
    for n in range(0, hidden, wide):
        total = jnp.dot(feats[:, :bulk], w_first[:bulk, n : n + wide], preferred_element_type=F32)
        total = total + jnp.dot(
            feats[:, bulk:depth], w_first[bulk:depth, n : n + wide], preferred_element_type=F32
        )
        preact[:, n : n + wide] = total + b_first[:, n : n + wide]

    def head_step(s, _):
        rows = pl.ds(pl.multiple_of(s * 16, 16), 16)
        v = preact[rows, :]
        squash = jax.nn.sigmoid(v)
        logit = jnp.sum(v * squash * w_out[...], axis=1, keepdims=True)
        logit_grad = jax.nn.sigmoid(logit) - labels[rows, :].astype(F32)
        slope = squash * (1.0 + v * (1.0 - squash))
        pre_grad[rows, :] = (logit_grad * w_out[...] * slope).astype(BF16)
        return 0

    lax.fori_loop(0, batch // 16, head_step, 0)

    bulk = pairs // wide * wide
    for n in range(0, pairs, wide):
        span = min(wide, pairs - n)
        g = lax.dot_general(
            pre_grad[...], w_first[n : n + span, :], (((1,), (1,)), ((), ())),
            preferred_element_type=F32,
        )
        pair_grad[:, n : n + span] = g * scale

    def unpack_step(s, _):
        rows = pl.ds(pl.multiple_of(s * part, part), part)
        offset = 0
        for i in range(pitch):
            where_to = pl.ds(s * (part * pitch) + i, part, stride=pitch)
            if i == 0 or i >= vec_count:
                gram[where_to, :] = jnp.zeros((part, LANES), F32)
                continue
            turn = offset % LANES
            number = offset // LANES
            back = (LANES - turn) % LANES
            piece = pair_grad[rows, number * LANES : (number + 1) * LANES]
            if back:
                piece = pltpu.roll(piece, back, 1)
            if turn + i > LANES:
                more = pair_grad[rows, (number + 1) * LANES : (number + 2) * LANES]
                piece = jnp.where(lane < LANES - turn, piece, pltpu.roll(more, back, 1))
            gram[where_to, :] = jnp.where(lane < i, piece, 0.0)
            offset += i
        return 0

    lax.fori_loop(0, batch // part, unpack_step, 0)

    def grad_step(s, _):
        base = s * (together * pitch)
        found = []
        for n in range(together):
            spot = pl.multiple_of(base + n * pitch, 8)
            lower = gram[pl.ds(spot, pitch), :]
            vectors = vec[pl.ds(spot, pitch), :].astype(BF16)
            found.append((lower, vectors))
        for n in range(together):
            lower, vectors = found[n]
            spot = pl.multiple_of(base + n * pitch, 8)
            both = (lower[:, :pitch] + jnp.transpose(lower)[:pitch, :]).astype(BF16)
            vec[pl.ds(spot, pitch), :] = jnp.dot(both, vectors, preferred_element_type=F32)
        return 0

    lax.fori_loop(0, batch // together, grad_step, 0)

    for t in range(small_count):
        small_out[t] = vec[column(1 + t), :].astype(BF16)
    sample_t = lax.broadcasted_iota(jnp.int32, (bags, batch), 1)
    bag_t = lax.broadcasted_iota(jnp.int32, (bags, batch), 0)
    for f in range(feat_count):
        hot = jnp.where(((sample_t * sizes[f]) >> shift) == bag_t, 1.0, 0.0).astype(BF16)
        grads = vec[column(first_large + f), :].astype(BF16)
        fold = jnp.dot(hot, grads, preferred_element_type=F32).astype(BF16)
        for copy in range(fold_out.shape[0]):
            fold_out[copy, f] = fold


def top(sizes, arrived, small, dense, labels, w_first, b_first, w_out, copies):
    feat_count, bags, width = arrived.shape
    small_count, batch, _ = small.shape
    vec_count = 1 + small_count + feat_count
    pitch = -(-vec_count // 8) * 8
    pairs = vec_count * (vec_count - 1) // 2
    depth = pairs + width
    hidden = w_first.shape[1]

    def up(n):
        return -(-n // LANES) * LANES

    return pl.pallas_call(
        functools.partial(top_kernel, pitch=pitch, vec_count=vec_count),
        out_shape=(
            jax.ShapeDtypeStruct((small_count, batch, width), BF16),
            jax.ShapeDtypeStruct((copies, feat_count, bags, width), BF16),
        ),
        in_specs=[whole(pltpu.SMEM)] + [whole()] * 4 + [whole(pl.ANY)] + [whole()] * 2,
        out_specs=(whole(), whole()),
        scratch_shapes=[
            pltpu.VMEM((batch * pitch + LANES - pitch, width), F32),
            pltpu.VMEM((batch * pitch, LANES), F32),
            pltpu.VMEM((batch, up(depth)), BF16),
            pltpu.VMEM((batch, hidden), F32),
            pltpu.VMEM((batch, hidden), BF16),
            pltpu.VMEM((batch, up(pairs)), F32),
            pltpu.VMEM(w_first.shape, BF16),
            pltpu.SemaphoreType.DMA,
        ],
        compiler_params=pltpu.CompilerParams(vmem_limit_bytes=VMEM_CAP),
        cost_estimate=cost(45),
        name="top",
    )(sizes, arrived, small, dense, labels, w_first, b_first, w_out)


def step(
    dense, small_ids, labels, small_tables, large_tables,
    batch_sizes, bag_ends, owner_row_index, w_first, b_first, w_out,
):
    groups = 1
    for name in OWNERS:
        groups = groups * lax.axis_size(name)
    copies = lax.axis_size("rep")
    me = lax.axis_index(ALL)
    small_rows = small_tables.shape[1]
    table = large_tables[0]
    ends = bag_ends[0]
    slots = owner_row_index.shape[2]
    flat_ends = ends.reshape(-1)
    ids = owner_row_index.reshape(-1, 8, slots // 128, 128).transpose(0, 2, 1, 3).reshape(-1)

    sizes = lax.dynamic_slice_in_dim(batch_sizes, me, 1, 1)[:, 0]

    arrived, small = pool_and_send(
        ids, ends, small_ids.T, table, small_tables, groups, slots
    )
    later_ids, arrived = lax.optimization_barrier((small_ids, arrived))
    ids_sent = lax.all_gather(later_ids.T, PLANE)
    ids_sent = lax.dynamic_index_in_dim(ids_sent, lax.axis_index(PLANE), 1, False)
    small_grad, folded = top(
        sizes, arrived, small, dense, labels[:, None], w_first, b_first[None], w_out[None], copies
    )

    grads = lax.all_to_all(small_grad, PLANE, 0, 0, tiled=True).reshape(-1, LANES)
    owner_hot = (ids_sent.reshape(-1)[:, None] == jnp.arange(small_rows, dtype=jnp.int32)).astype(BF16)
    partial = jnp.einsum("sr,se->re", owner_hot, grads, preferred_element_type=F32)
    found = lax.all_gather(partial.astype(BF16), "x")
    total = found.astype(F32).sum(0)
    table_index = lax.axis_index(PLANE)
    mine_small = lax.dynamic_slice_in_dim(small_tables, table_index, 1, 0)[0]
    new_small = (mine_small.astype(F32) - step_size * total).astype(BF16)
    small_new = lax.all_gather(new_small, PLANE)

    folds = lax.all_to_all(folded.reshape((-1,) + folded.shape[2:]), ALL, 0, 0, tiled=True)
    large_new = scatter(ids, flat_ends, ends, folds, table, slots)
    return small_new, large_new[None]


def solution(mesh):
    fine = Mesh(mesh.devices.reshape(2, 4, 2, 4, 2), ALL)
    placed = (
        P(ALL, None), P(ALL, None), P(ALL), P(), P(OWNERS, None, None), P(),
        P(OWNERS, None, None), P(OWNERS, None, None), P(), P(), P(),
    )
    return jax.shard_map(
        step, mesh=fine, in_specs=placed, out_specs=(P(), P(OWNERS, None, None)), check_vma=False
    )
```
